16 devices in a mesh: rep: 1, r: 2 (over z), s: 8 (over x, y, core).
Axes of the slice: x: 2, y: 2, z: 2, core: 2. Of those that a mesh axis runs over, the one named last changes fastest.
Arguments:
- x: bfloat16 [16, 4096, 896], P(('rep', 'r', 's'))
- dy: bfloat16 [16, 4096, 896], P(('rep', 'r', 's'))
- w_gate: bfloat16 [2, 896, 2304], P(None, 's')
- w_up: bfloat16 [2, 896, 2304], P(None, 's')
- w_down: bfloat16 [2, 2304, 896], P(None, 's')
- m_w_gate: float32 [2, 896, 2304], P(None, 's')
- m_w_up: float32 [2, 896, 2304], P(None, 's')
- m_w_down: float32 [2, 2304, 896], P(None, 's')
- v_w_gate: float32 [2, 896, 2304], P(None, 's')
- v_w_up: float32 [2, 896, 2304], P(None, 's')
- v_w_down: float32 [2, 2304, 896], P(None, 's')
Outputs:
- output 1: bfloat16 [2, 896, 2304], P('rep', 's')
- output 2: bfloat16 [2, 896, 2304], P('rep', 's')
- output 3: bfloat16 [2, 2304, 896], P('rep', 's')
- output 4: float32 [2, 896, 2304], P('rep', 's')
- output 5: float32 [2, 896, 2304], P('rep', 's')
- output 6: float32 [2, 2304, 896], P('rep', 's')
- output 7: float32 [2, 896, 2304], P('rep', 's')
- output 8: float32 [2, 896, 2304], P('rep', 's')
- output 9: float32 [2, 2304, 896], P('rep', 's')
All inputs are finite; a program needn't handle non-finite values.
Results may differ from the reference program's by a relative error of at most 0.022.
Values are sent between devices in bfloat16 or wider.
A program may use at most 2 GiB of HBM per device.

```python
import jax
import jax.numpy as jnp
from jax import lax

SEQUENCES = 16
TOKENS = 4096
D = 896
FF = 2304
LAYERS = 2
NAMES = ("w_gate", "w_up", "w_down")
SHAPES = {"w_gate": (LAYERS, D, FF), "w_up": (LAYERS, D, FF), "w_down": (LAYERS, FF, D)}


def bump(key, n, height):
    away = (jnp.arange(n, dtype=jnp.int32) - jax.random.randint(key, (), 0, n, jnp.int32)) % n
    return jnp.where(away < n // 8, height, 1.0)


def together(key, own, strength):
    shared = jax.random.normal(key, own.shape[1:], jnp.float32)
    return (own + strength * shared) * lax.rsqrt(1 + strength * strength)


def setup_inputs(seed: int = 0, part: int = 0) -> dict:
    kx, kdy, ka, kb, kz, kf, kh, kl, *keys = jax.random.split(jax.random.key(seed), 8 + 3 * len(NAMES))
    kx, kdy, ka, kb = (jax.random.fold_in(k, part) for k in (kx, kdy, ka, kb))
    kw, km, kv = (keys[i::3] for i in range(3))
    shape = (SEQUENCES, TOKENS, D)
    much_x, much_dy = jax.random.uniform(kz, (2,), jnp.float32, 0.0, 1.0)
    loud = 2.0 ** jax.random.uniform(jax.random.fold_in(kz, 1), (), jnp.float32, -1.0, 2.0)
    layers = 2.0 ** jax.random.uniform(kl, (LAYERS, 1, 1), jnp.float32, -1.0, 1.0)
    x = together(ka, jax.random.normal(kx, shape, jnp.float32), much_x) * bump(kf, D, 4.0)
    dy = together(kb, jax.random.normal(kdy, shape, jnp.float32), much_dy)
    drawn = {"x": x.astype(jnp.bfloat16), "dy": (loud * dy * (SEQUENCES * TOKENS) ** -0.5).astype(jnp.bfloat16)}
    for key, name in zip(kw, NAMES, strict=True):
        w = jax.random.normal(key, SHAPES[name], jnp.float32) * SHAPES[name][1] ** -0.5
        drawn[name] = (w * {"w_gate": 1.0, "w_up": bump(kh, FF, 4.0), "w_down": layers}[name]).astype(jnp.bfloat16)
    for key, name in zip(km, NAMES, strict=True):
        drawn[f"m_{name}"] = 0.1 * jax.random.normal(key, SHAPES[name], jnp.float32)
    for key, name in zip(kv, NAMES, strict=True):
        drawn[f"v_{name}"] = jax.random.uniform(key, SHAPES[name], jnp.float32, 0.005, 0.015)
    return drawn


def matmul(a, w):
    return jnp.dot(a, w, preferred_element_type=jnp.float32).astype(jnp.bfloat16)


def normed(h):
    wide = h.astype(jnp.float32)
    scale = lax.rsqrt(jnp.mean(wide**2, -1, keepdims=True) + 1e-6)
    return (wide * scale).astype(jnp.bfloat16)


def layer(h, w):
    a = normed(h)
    gate = jnp.dot(a, w["w_gate"], preferred_element_type=jnp.float32)
    up = jnp.dot(a, w["w_up"], preferred_element_type=jnp.float32)
    return h + matmul((jax.nn.silu(gate) * up).astype(jnp.bfloat16), w["w_down"])


def adamw(w, m, v, g):
    m = 0.9 * m + 0.1 * g
    v = 0.95 * v + 0.05 * g * g
    step = m * lax.rsqrt(v + 1e-8) + 0.1 * w
    return (w - 0.02 * step).astype(jnp.bfloat16), m, v


def clipped(gradients, sum_of_squares, count):
    factor = jnp.minimum(1.0, 0.5 * lax.rsqrt(sum_of_squares / count + 1e-30))
    return [g * factor for g in gradients]


def stack(weights, h):
    return lax.scan(lambda h, w: (layer(h, w), None), h, weights)[0]


def reference(x, dy, w_gate, w_up, w_down, m_w_gate, m_w_up, m_w_down, v_w_gate, v_w_up, v_w_down):
    weights = dict(zip(NAMES, (w_gate, w_up, w_down), strict=True))

    def take(so_far, sequence):
        h, by_y = sequence
        _, back = jax.vjp(lambda w: stack(w, h), weights)
        return jax.tree.map(lambda total, term: total + term.astype(jnp.float32), so_far, back(by_y)[0]), None

    none_yet = {name: jnp.zeros(w.shape, jnp.float32) for name, w in weights.items()}
    by_weights, _ = lax.scan(take, none_yet, (x, dy))
    gradients = [by_weights[name].astype(jnp.bfloat16).astype(jnp.float32) for name in NAMES]
    gradients = clipped(gradients, sum(jnp.sum(g * g) for g in gradients), sum(g.size for g in gradients))
    new = [
        adamw(w.astype(jnp.float32), m, v, g)
        for w, m, v, g in zip((w_gate, w_up, w_down), (m_w_gate, m_w_up, m_w_down), (v_w_gate, v_w_up, v_w_down), gradients, strict=True)
    ]
    return tuple(one[which] for which in range(3) for one in new)
```

```python
import functools

import jax
import jax.numpy as jnp
from jax import lax
from jax.experimental import pallas as pl
from jax.experimental.pallas import tpu as pltpu
from jax.sharding import PartitionSpec as P

NAMES = ("w_gate", "w_up", "w_down")
MESH = pl.DeviceIdType.MESH
BF, F32 = jnp.bfloat16, jnp.float32
LIMIT = 60 * 1024 * 1024
LANES = 128


def wide(a):
    return a.astype(F32)


def dot(a, b, contract=((1,), (0,))):
    return lax.dot_general(a, b, (contract, ((), ())), preferred_element_type=F32)


def scale_of(h):
    return lax.rsqrt(jnp.mean(h * h, -1, keepdims=True) + 1e-6)


class Place:
    def __init__(self):
        s = lax.axis_index("s")
        x, y, core = s // 4, (s // 2) % 2, s % 2
        at = lambda x, y, core: x * 4 + y * 2 + core
        self.s, self.z = s, lax.axis_index("r")
        self.other, self.xn, self.yn, self.diagonal = at(x, y, 1 - core), at(1 - x, y, core), at(x, 1 - y, core), at(1 - x, 1 - y, core)

    def neighbours(self):
        return ({"s": self.other}, {"s": self.xn}, {"s": self.yn}, {"r": 1 - self.z})

    def barrier(self):
        barrier = pltpu.get_barrier_semaphore()
        for device in self.neighbours():
            pl.semaphore_signal(barrier, inc=1, device_id=device, device_id_type=MESH)
        pl.semaphore_wait(barrier, 4)


TRANSFERS = 13


class Gather:
    def __init__(self, place, block, whole, split, sems):
        self.p, self.block, self.whole = place, block, whole
        self.rows = block.shape[0]
        self.axis, first, second = split
        self.parts = ((0, first), (first, second))
        self.half = first + second
        self.send, self.recv, self.local = sems

    def at(self, s):
        return self.whole.at[pl.ds(pl.multiple_of(s * self.rows, 16), self.rows)]

    def part(self, s, z, which):
        start, size = self.parts[which]
        offset = z * self.half + start
        if self.axis == 1:
            return self.at(s).at[:, pl.ds(pl.multiple_of(offset, LANES), size)]
        return self.whole.at[pl.ds(pl.multiple_of(s * self.rows + offset, 16), size)]

    def copy(self, k):
        p, z = self.p, self.p.z
        core, xn, yn, zn = self.p.neighbours()
        source, target, device = {
            0: lambda: (self.block, self.at(p.s), core),
            1: lambda: (self.block, self.at(p.s), xn),
            2: lambda: (self.block, self.at(p.s), yn),
            3: lambda: (self.at(p.xn), self.at(p.xn), core),
            4: lambda: (self.at(p.yn), self.at(p.yn), core),
            5: lambda: (self.part(p.xn, z, 0), self.part(p.xn, z, 0), yn),
            6: lambda: (self.part(p.yn, z, 1), self.part(p.yn, z, 1), xn),
            7: lambda: (self.part(p.diagonal, z, 0), self.part(p.diagonal, z, 0), zn),
            8: lambda: (self.part(p.diagonal, z, 1), self.part(p.diagonal, z, 1), zn),
            9: lambda: (self.part(p.diagonal, z, 0), self.part(p.diagonal, z, 0), core),
            10: lambda: (self.part(p.diagonal, z, 1), self.part(p.diagonal, z, 1), core),
            11: lambda: (self.part(p.diagonal, 1 - z, 0), self.part(p.diagonal, 1 - z, 0), core),
            12: lambda: (self.part(p.diagonal, 1 - z, 1), self.part(p.diagonal, 1 - z, 1), core),
        }[k]()
        return pltpu.make_async_remote_copy(
            src_ref=source, dst_ref=target, send_sem=self.send.at[k], recv_sem=self.recv.at[k], device_id=device, device_id_type=MESH
        )

    def keep(self):
        return pltpu.make_async_copy(self.block, self.at(self.p.s), self.local)

    def start(self):
        for k in (1, 2, 0):
            self.copy(k).start()
        self.keep().start()

    def passing(self, after, then):
        self.copy(after).wait_recv()
        for k in then:
            self.copy(k).start()

    def second(self):
        self.passing(1, (5, 3))
        self.passing(2, (6, 4))

    def third(self):
        self.passing(5, (7, 9))
        self.passing(6, (8, 10))

    def fourth(self):
        self.passing(7, (11,))
        self.passing(8, (12,))

    def finish(self):
        for k in (0, 3, 4, 9, 10, 11, 12):
            self.copy(k).wait_recv()
        for k in range(TRANSFERS):
            self.copy(k).wait_send()
        self.keep().wait()


def gather_sems(jobs):
    return [pltpu.SemaphoreType.DMA((jobs, TRANSFERS)), pltpu.SemaphoreType.DMA((jobs, TRANSFERS)), pltpu.SemaphoreType.DMA((jobs,))]


def halves_of(columns):
    half = columns // 2
    first = (half // LANES + 1) // 2 * LANES
    return first, half - first


def on(step, *actions):
    @pl.when(step)
    def _():
        for action in actions:
            action()


def sigmoid(x):
    return 0.5 * jnp.tanh(0.5 * x) + 0.5


def gate_up_kernel(parts, tiles, h_ref, wg_ref, wu_ref, wd_ref, g_ref, u_ref, hid_ref, at_ref, wd0_ref, wg1_ref, wg, wu, send, recv, local):
    part, tile = pl.program_id(0), pl.program_id(1)
    step = part * tiles + tile
    place = Place()
    width = g_ref.shape[1]
    sems = lambda j: (send.at[j], recv.at[j], local.at[j])
    jobs = []
    for n in range(parts):
        cols = pl.ds(n * width, width)
        for i, (own, whole) in enumerate(((wg_ref, wg), (wu_ref, wu))):
            jobs.append(Gather(place, own.at[0, :, cols], whole.at[:, cols], (1, *halves_of(width)), sems(2 * n + i)))
    rows = wd_ref.shape[1]
    down = Gather(place, wd_ref.at[0], wd0_ref, (0, (rows // 2 // 16 + 1) // 2 * 16, rows // 2 - (rows // 2 // 16 + 1) // 2 * 16), sems(2 * parts))
    nxt = Gather(place, wg_ref.at[1], wg1_ref, (1, *halves_of(wg_ref.shape[2])), sems(2 * parts + 1))
    b = lambda n, what: [getattr(jobs[2 * n + i], what) for i in range(2)]
    last = parts * tiles - 1

    on(step == 0, place.barrier, *b(0, "start"), *b(0, "second"), *b(1, "start"), *b(0, "third"), *b(0, "fourth"), *b(0, "finish"))
    on(step == 4, *b(1, "second"), *b(2, "start"))
    on(step == 5, *b(1, "third"))
    on(step == 7, *b(1, "fourth"))
    on(step == 8, *b(1, "finish"))
    on(step == 10, *b(2, "second"), down.start)
    on(step == 12, *b(2, "third"))
    on(step == 14, *b(2, "fourth"))
    on(step == 16, *b(2, "finish"))
    on(step == 17, down.second, nxt.start)
    on(step == 19, down.third)
    on(step == 20, down.fourth)
    on(step == 22, nxt.second, down.finish)

    h = wide(h_ref[...])
    a = (h * scale_of(h)).astype(BF)

    @pl.when(part == 0)
    def _():
        at_ref[...] = a.T

    for n in range(0, width, 256):
        where = pl.ds(pl.multiple_of(part * width + n, LANES), 256)
        g = dot(a, wg[:, where])
        u = dot(a, wu[:, where])
        g_ref[:, n : n + 256] = g
        u_ref[:, n : n + 256] = u
        hid_ref[:, n : n + 256] = (g * sigmoid(g) * u).astype(BF)

    on(step == last, nxt.third, nxt.fourth, nxt.finish)


def gate_up(h, wg, wu, wd):
    tokens, d = h.shape
    _, rows, f = wg.shape
    parts, tile = 3, 512
    width, tiles = f // parts, tokens // tile
    group = d // rows
    any_ = pl.BlockSpec(memory_space=pl.ANY)
    return pl.pallas_call(
        functools.partial(gate_up_kernel, parts, tiles),
        grid=(parts, tiles),
        out_shape=[
            jax.ShapeDtypeStruct((tokens, f), F32),
            jax.ShapeDtypeStruct((tokens, f), F32),
            jax.ShapeDtypeStruct((tokens, f), BF),
            jax.ShapeDtypeStruct((d, tokens), BF),
            jax.ShapeDtypeStruct((wd.shape[1] * group, d), BF),
            jax.ShapeDtypeStruct((d, f), BF),
        ],
        in_specs=[pl.BlockSpec((tile, d), lambda p, t: (t, 0)), any_, any_, any_],
        out_specs=[pl.BlockSpec((tile, width), lambda p, t: (t, p))] * 3
        + [pl.BlockSpec((d, tile), lambda p, t: (0, jnp.where(p == 0, t, tiles - 1))), any_, any_],
        scratch_shapes=[pltpu.VMEM((d, f), BF)] * 2 + gather_sems(2 * parts + 2),
        compiler_params=pltpu.CompilerParams(
            collective_id=0, has_side_effects=True, vmem_limit_bytes=LIMIT, dimension_semantics=("arbitrary", "arbitrary")
        ),
        cost_estimate=pl.CostEstimate(flops=4 * tokens * d * f, bytes_accessed=110_000_000, transcendentals=tokens * f),
        name="gate_up",
    )(h, wg, wu, wd)


def down_kernel(tiles, hid_ref, h_ref, w_ref, wu_ref, wd_ref, h1_ref, wu1_ref, wd1_ref, send, recv, local):
    step = pl.program_id(0)
    place = Place()
    sems = lambda j: (send.at[j], recv.at[j], local.at[j])
    rows = wd_ref.shape[1]
    up = Gather(place, wu_ref.at[1], wu1_ref, (1, *halves_of(wu_ref.shape[2])), sems(0))
    down = Gather(place, wd_ref.at[1], wd1_ref, (0, (rows // 2 // 16 + 1) // 2 * 16, rows // 2 - (rows // 2 // 16 + 1) // 2 * 16), sems(1))
    on(step == 0, place.barrier, up.start)
    on(step == tiles // 2, up.second, down.start)
    on(step == tiles // 2 + 2, up.third)
    h1_ref[...] = h_ref[...] + dot(hid_ref[...], w_ref[...]).astype(BF)
    on(step == tiles - 1, up.fourth, down.second, up.finish, down.third, down.fourth, down.finish)


def down(hid, h, w, wu, wd):
    tokens, d = h.shape
    f = hid.shape[1]
    tile = 512
    any_ = pl.BlockSpec(memory_space=pl.ANY)
    return pl.pallas_call(
        functools.partial(down_kernel, tokens // tile),
        grid=(tokens // tile,),
        out_shape=[jax.ShapeDtypeStruct((tokens, d), BF), jax.ShapeDtypeStruct((d, f), BF), jax.ShapeDtypeStruct((f, d), BF)],
        in_specs=[
            pl.BlockSpec((tile, f), lambda t: (t, 0)),
            pl.BlockSpec((tile, d), lambda t: (t, 0)),
            pl.BlockSpec((f, d), lambda t: (0, 0), pipeline_mode=pl.Buffered(1)),
            any_,
            any_,
        ],
        out_specs=[pl.BlockSpec((tile, d), lambda t: (t, 0)), any_, any_],
        scratch_shapes=gather_sems(2),
        compiler_params=pltpu.CompilerParams(collective_id=1, has_side_effects=True, vmem_limit_bytes=LIMIT, dimension_semantics=("arbitrary",)),
        cost_estimate=pl.CostEstimate(flops=2 * tokens * d * f, bytes_accessed=37_000_000, transcendentals=0),
        name="down",
    )(hid, h, w, wu, wd)


def last_kernel(h_ref, dy_ref, wg_ref, wu_ref, wd_ref, hid_ref, dg_ref, du_ref, at_ref, dyt_ref, dh_ref, dht_ref):
    h = wide(h_ref[...])
    scale = scale_of(h)
    a = (h * scale).astype(BF)
    dy = dy_ref[...]
    at_ref[...] = a.T
    dyt_ref[...] = dy.T
    f = wg_ref.shape[1]
    by_a = jnp.zeros(h.shape, F32)
    for n in range(0, f, 768):
        for k in range(n, n + 768, 256):
            where = slice(k, k + 256)
            g = dot(a, wg_ref[:, where])
            u = dot(a, wu_ref[:, where])
            back = wide(dot(dy, wd_ref[where, :], ((1,), (1,))).astype(BF))
            s = sigmoid(g)
            silu = g * s
            hid_ref[:, where] = (silu * u).astype(BF)
            du_ref[:, where] = (back * silu).astype(BF)
            dg_ref[:, where] = (back * u * (s * (1.0 + g * (1.0 - s)))).astype(BF)
        where = slice(n, n + 768)
        by_a += dot(dg_ref[:, where], wg_ref[:, where], ((1,), (1,))) + dot(du_ref[:, where], wu_ref[:, where], ((1,), (1,)))
    by_a = wide(by_a.astype(BF))
    mean = jnp.mean(by_a * h, -1, keepdims=True)
    by_h = (by_a * scale - h * (scale * scale * scale * mean)).astype(BF)
    by_h = dy + by_h
    dh_ref[...] = by_h
    dht_ref[...] = by_h.T


def last_layer(h, dy, wg, wu, wd):
    tokens, d = h.shape
    f = wg.shape[1]
    tile = 512
    rows = lambda n: pl.BlockSpec((tile, n), lambda t: (t, 0))
    columns = pl.BlockSpec((d, tile), lambda t: (0, t))
    fixed = lambda m, n: pl.BlockSpec((m, n), lambda t: (0, 0), pipeline_mode=pl.Buffered(1))
    shape = lambda *s: jax.ShapeDtypeStruct(s, BF)
    return pl.pallas_call(
        last_kernel,
        grid=(tokens // tile,),
        out_shape=[shape(tokens, f)] * 3 + [shape(d, tokens)] * 2 + [shape(tokens, d), shape(d, tokens)],
        in_specs=[rows(d), rows(d), fixed(d, f), fixed(d, f), fixed(f, d)],
        out_specs=[rows(f)] * 3 + [columns] * 2 + [rows(d), columns],
        compiler_params=pltpu.CompilerParams(vmem_limit_bytes=LIMIT, dimension_semantics=("arbitrary",)),
        cost_estimate=pl.CostEstimate(flops=10 * tokens * d * f, bytes_accessed=110_000_000, transcendentals=tokens * f),
        name="last_layer",
    )(h, dy, wg, wu, wd)


def back_kernel(dh_ref, g_ref, u_ref, wd_ref, dg_ref, du_ref):
    dh = dh_ref[...]
    for k in range(0, g_ref.shape[1], 256):
        where = slice(k, k + 256)
        back = wide(dot(dh, wd_ref[where, :], ((1,), (1,))).astype(BF))
        g, u = g_ref[:, where], u_ref[:, where]
        s = sigmoid(g)
        du_ref[:, where] = (back * (g * s)).astype(BF)
        dg_ref[:, where] = (back * u * (s * (1.0 + g * (1.0 - s)))).astype(BF)


def back_to_hidden(dh, g, u, wd):
    tokens, d = dh.shape
    f = g.shape[1]
    tile = 256
    rows = lambda n: pl.BlockSpec((tile, n), lambda t: (t, 0))
    return pl.pallas_call(
        back_kernel,
        grid=(tokens // tile,),
        out_shape=[jax.ShapeDtypeStruct((tokens, f), BF)] * 2,
        in_specs=[rows(d), rows(f), rows(f), pl.BlockSpec((f, d), lambda t: (0, 0), pipeline_mode=pl.Buffered(1))],
        out_specs=[rows(f)] * 2,
        compiler_params=pltpu.CompilerParams(vmem_limit_bytes=LIMIT, dimension_semantics=("arbitrary",)),
        cost_estimate=pl.CostEstimate(flops=2 * tokens * d * f, bytes_accessed=125_000_000, transcendentals=tokens * f),
        name="back_to_hidden",
    )(dh, g, u, wd)


def term_kernel(turned, left_ref, right_ref, out_ref):
    total = dot(left_ref[...], right_ref[...])
    out_ref[...] = (total.T if turned else total).astype(BF)


def term(left, right, turned):
    d, tokens = left.shape
    f = right.shape[1]
    width = 768
    return pl.pallas_call(
        functools.partial(term_kernel, turned),
        grid=(f // width,),
        out_shape=jax.ShapeDtypeStruct((f, d) if turned else (d, f), BF),
        in_specs=[
            pl.BlockSpec((d, tokens), lambda n: (0, 0), pipeline_mode=pl.Buffered(1)),
            pl.BlockSpec((tokens, width), lambda n: (0, n)),
        ],
        out_specs=pl.BlockSpec((width, d), lambda n: (n, 0)) if turned else pl.BlockSpec((d, width), lambda n: (0, n)),
        compiler_params=pltpu.CompilerParams(vmem_limit_bytes=LIMIT, dimension_semantics=("arbitrary",)),
        cost_estimate=pl.CostEstimate(flops=2 * tokens * d * f, bytes_accessed=30_000_000, transcendentals=0),
        name="term_turned" if turned else "term",
    )(left, right)


def adamw(w, m, v, g):
    m = 0.9 * m + 0.1 * g
    v = 0.95 * v + 0.05 * g * g
    step = m * lax.rsqrt(v + 1e-8) + 0.1 * w
    return (w - 0.02 * step).astype(jnp.bfloat16), m, v


def clipped(gradients, sum_of_squares, count):
    factor = jnp.minimum(1.0, 0.5 * lax.rsqrt(sum_of_squares / count + 1e-30))
    return [g * factor for g in gradients]


def flip(a, bit):
    return lax.ppermute(a, "s", [(i, i ^ bit) for i in range(8)])


def summed(term, x_first):
    rows, columns = term.shape
    place = lax.axis_index("s")
    x, y, core = place // 4, place // 2 % 2, place % 2
    blocks = term.reshape(2, 2, 2, rows // 8, columns)
    (first, a, abit), (second, b, bbit) = ((0, x, 4), (1, y, 2)) if x_first else ((1, y, 2), (0, x, 4))
    del second

    def pick(array, axis, index):
        return lax.dynamic_index_in_dim(array, index, axis, keepdims=False)

    from_core = flip(pick(blocks, 2, 1 - core), 1)
    mine = pick(blocks, 2, core)

    def two(index):
        return wide(pick(mine, first, index)) + wide(pick(from_core, first, index))

    from_first = flip(two(1 - a).astype(jnp.bfloat16), abit)

    def four(index):
        return (
            wide(pick(pick(mine, first, a), 0, index))
            + wide(pick(pick(from_core, first, a), 0, index))
            + wide(pick(from_first, 0, index))
        )

    from_second = flip(four(1 - b).astype(jnp.bfloat16), bbit)
    eight = (four(b) + wide(from_second)).astype(jnp.bfloat16)
    other = lax.ppermute(eight, "r", [(0, 1), (1, 0)])
    return (wide(eight) + wide(other)).astype(jnp.bfloat16)


def solution(mesh):
    def step(x, dy, *arrays):
        weights, m, v = (arrays[i : i + 3] for i in (0, 3, 6))
        layers = weights[0].shape[0]
        wg, wu, wd = weights
        x, dy = x[0], dy[0]
        g, u, hid0, at0, wd0, wg1 = gate_up(x, wg, wu, wd)
        h, wu1, wd1 = down(hid0, x, wd0, wu, wd)
        hid1, dg1, du1, at1, dyt, dh, dht = last_layer(h, dy, wg1, wu1, wd1)
        mine = [[None] * 3 for _ in range(layers)]
        mine[1][2] = summed(term(dyt, hid1, True), True)
        mine[1][0] = summed(term(at1, dg1, False), False)
        mine[1][1] = summed(term(at1, du1, False), True)
        mine[0][2] = summed(term(dht, hid0, True), False)
        dg0, du0 = back_to_hidden(dh, g, u, wd0)
        mine[0][0] = summed(term(at0, dg0, False), True)
        mine[0][1] = summed(term(at0, du0, False), False)
        gradients = [jnp.stack([mine[number][i] for number in range(layers)]).astype(F32) for i in range(3)]
        squares = lax.psum(sum(jnp.sum(g * g) for g in gradients), "s")
        gradients = clipped(gradients, squares, lax.psum(1, "s") * sum(g.size for g in gradients))
        new = [adamw(w.astype(F32), m, v, g) for w, m, v, g in zip(weights, m, v, gradients, strict=True)]
        return tuple(one[which] for which in range(3) for one in new)

    states, cut = P(("rep", "r", "s"), None, None), P(None, "s", None)
    return jax.shard_map(
        step,
        mesh=mesh,
        in_specs=(states, states) + (cut,) * 9,
        out_specs=(P("rep", "s", None),) * 9,
        check_vma=False,
    )
```

```python
import functools

import jax
import jax.numpy as jnp
from jax import lax
from jax.experimental import pallas as pl
from jax.experimental.pallas import tpu as pltpu
from jax.sharding import PartitionSpec as P

NAMES = ("w_gate", "w_up", "w_down")
MESH = pl.DeviceIdType.MESH
BF, F32 = jnp.bfloat16, jnp.float32
LIMIT = 60 * 1024 * 1024
LANES = 128


def wide(a):
    return a.astype(F32)


def dot(a, b, contract=((1,), (0,))):
    return lax.dot_general(a, b, (contract, ((), ())), preferred_element_type=F32)


def scale_of(h):
    return lax.rsqrt(jnp.mean(h * h, -1, keepdims=True) + 1e-6)


class Place:
    def __init__(self):
        s = lax.axis_index("s")
        x, y, core = s // 4, (s // 2) % 2, s % 2
        at = lambda x, y, core: x * 4 + y * 2 + core
        self.s, self.z = s, lax.axis_index("r")
        self.other, self.xn, self.yn, self.diagonal = at(x, y, 1 - core), at(1 - x, y, core), at(x, 1 - y, core), at(1 - x, 1 - y, core)

    def neighbours(self):
        return ({"s": self.other}, {"s": self.xn}, {"s": self.yn}, {"r": 1 - self.z})

    def barrier(self):
        barrier = pltpu.get_barrier_semaphore()
        for device in self.neighbours():
            pl.semaphore_signal(barrier, inc=1, device_id=device, device_id_type=MESH)
        pl.semaphore_wait(barrier, 4)


TRANSFERS = 13


class Gather:
    def __init__(self, place, block, whole, split, sems):
        self.p, self.block, self.whole = place, block, whole
        self.rows = block.shape[0]
        self.axis, first, second = split
        self.parts = ((0, first), (first, second))
        self.half = first + second
        self.send, self.recv, self.local = sems

    def at(self, s):
        return self.whole.at[pl.ds(pl.multiple_of(s * self.rows, 16), self.rows)]

    def part(self, s, z, which):
        start, size = self.parts[which]
        offset = z * self.half + start
        if self.axis == 1:
            return self.at(s).at[:, pl.ds(pl.multiple_of(offset, LANES), size)]
        return self.whole.at[pl.ds(pl.multiple_of(s * self.rows + offset, 16), size)]

    def copy(self, k):
        p, z = self.p, self.p.z
        core, xn, yn, zn = self.p.neighbours()
        source, target, device = {
            0: lambda: (self.block, self.at(p.s), core),
            1: lambda: (self.block, self.at(p.s), xn),
            2: lambda: (self.block, self.at(p.s), yn),
            3: lambda: (self.at(p.xn), self.at(p.xn), core),
            4: lambda: (self.at(p.yn), self.at(p.yn), core),
            5: lambda: (self.part(p.xn, z, 0), self.part(p.xn, z, 0), yn),
            6: lambda: (self.part(p.yn, z, 1), self.part(p.yn, z, 1), xn),
            7: lambda: (self.part(p.diagonal, z, 0), self.part(p.diagonal, z, 0), zn),
            8: lambda: (self.part(p.diagonal, z, 1), self.part(p.diagonal, z, 1), zn),
            9: lambda: (self.part(p.diagonal, z, 0), self.part(p.diagonal, z, 0), core),
            10: lambda: (self.part(p.diagonal, z, 1), self.part(p.diagonal, z, 1), core),
            11: lambda: (self.part(p.diagonal, 1 - z, 0), self.part(p.diagonal, 1 - z, 0), core),
            12: lambda: (self.part(p.diagonal, 1 - z, 1), self.part(p.diagonal, 1 - z, 1), core),
        }[k]()
        return pltpu.make_async_remote_copy(
            src_ref=source, dst_ref=target, send_sem=self.send.at[k], recv_sem=self.recv.at[k], device_id=device, device_id_type=MESH
        )

    def keep(self):
        return pltpu.make_async_copy(self.block, self.at(self.p.s), self.local)

    def start(self):
        for k in (1, 2, 0):
            self.copy(k).start()
        self.keep().start()

    def passing(self, after, then):
        self.copy(after).wait_recv()
        for k in then:
            self.copy(k).start()

    def second(self):
        self.passing(1, (5, 3))
        self.passing(2, (6, 4))

    def third(self):
        self.passing(5, (7, 9))
        self.passing(6, (8, 10))

    def fourth(self):
        self.passing(7, (11,))
        self.passing(8, (12,))

    def finish(self):
        for k in (0, 3, 4, 9, 10, 11, 12):
            self.copy(k).wait_recv()
        for k in range(TRANSFERS):
            self.copy(k).wait_send()
        self.keep().wait()


def gather_sems(jobs):
    return [pltpu.SemaphoreType.DMA((jobs, TRANSFERS)), pltpu.SemaphoreType.DMA((jobs, TRANSFERS)), pltpu.SemaphoreType.DMA((jobs,))]


def halves_of(columns):
    half = columns // 2
    first = (half // LANES + 1) // 2 * LANES
    return first, half - first


def on(step, *actions):
    @pl.when(step)
    def _():
        for action in actions:
            action()


def sigmoid(x):
    return 0.5 * jnp.tanh(0.5 * x) + 0.5


def gate_up_kernel(parts, tiles, h_ref, wg_ref, wu_ref, wd_ref, g_ref, u_ref, hid_ref, at_ref, wd0_ref, wg1_ref, wu1_ref, wg, wu, send, recv, local):
    part, tile = pl.program_id(0), pl.program_id(1)
    step = part * tiles + tile
    place = Place()
    width = g_ref.shape[1]
    sems = lambda j: (send.at[j], recv.at[j], local.at[j])
    jobs = []
    for n in range(parts):
        cols = pl.ds(n * width, width)
        for i, (own, whole) in enumerate(((wg_ref, wg), (wu_ref, wu))):
            jobs.append(Gather(place, own.at[0, :, cols], whole.at[:, cols], (1, *halves_of(width)), sems(2 * n + i)))
    rows = wd_ref.shape[1]
    down = Gather(place, wd_ref.at[0], wd0_ref, (0, (rows // 2 // 16 + 1) // 2 * 16, rows // 2 - (rows // 2 // 16 + 1) // 2 * 16), sems(2 * parts))
    gate1 = Gather(place, wg_ref.at[1], wg1_ref, (1, *halves_of(wg_ref.shape[2])), sems(2 * parts + 1))
    up1 = Gather(place, wu_ref.at[1], wu1_ref, (1, *halves_of(wu_ref.shape[2])), sems(2 * parts + 2))
    b = lambda n, what: [getattr(jobs[2 * n + i], what) for i in range(2)]
    last = parts * tiles - 1

    on(
        step == 0,
        place.barrier,
        *b(0, "start"),
        *b(0, "second"),
        *b(1, "start"),
        *b(0, "third"),
        *b(0, "fourth"),
        *b(0, "finish"),
        *b(1, "second"),
        *b(2, "start"),
    )
    on(step == 2, *b(1, "third"))
    on(step == 3, *b(1, "fourth"))
    on(step == 4, down.start)
    on(step == 5, *b(2, "second"))
    on(step == 7, *b(2, "third"))
    on(step == 8, *b(1, "finish"))
    on(step == 9, *b(2, "fourth"), gate1.start)
    on(step == 11, down.second)
    on(step == 13, down.third)
    on(step == 14, up1.start)
    on(step == 15, down.fourth)
    on(step == 16, *b(2, "finish"))
    on(step == 17, gate1.second, down.finish)
    on(step == 19, gate1.third)
    on(step == 21, gate1.fourth)
    on(step == 22, up1.second, gate1.finish)

    h = wide(h_ref[...])
    a = (h * scale_of(h)).astype(BF)

    @pl.when(part == 0)
    def _():
        at_ref[...] = a.T

    for n in range(0, width, 256):
        where = pl.ds(pl.multiple_of(part * width + n, LANES), 256)
        g = dot(a, wg[:, where])
        u = dot(a, wu[:, where])
        g_ref[:, n : n + 256] = g
        u_ref[:, n : n + 256] = u
        hid_ref[:, n : n + 256] = (g * sigmoid(g) * u).astype(BF)

    on(step == last, up1.third, up1.fourth, up1.finish)


def gate_up(h, wg, wu, wd):
    tokens, d = h.shape
    _, rows, f = wg.shape
    parts, tile = 3, 512
    width, tiles = f // parts, tokens // tile
    group = d // rows
    any_ = pl.BlockSpec(memory_space=pl.ANY)
    return pl.pallas_call(
        functools.partial(gate_up_kernel, parts, tiles),
        grid=(parts, tiles),
        out_shape=[
            jax.ShapeDtypeStruct((tokens, f), F32),
            jax.ShapeDtypeStruct((tokens, f), F32),
            jax.ShapeDtypeStruct((tokens, f), BF),
            jax.ShapeDtypeStruct((d, tokens), BF),
            jax.ShapeDtypeStruct((wd.shape[1] * group, d), BF),
            jax.ShapeDtypeStruct((d, f), BF),
            jax.ShapeDtypeStruct((d, f), BF),
        ],
        in_specs=[pl.BlockSpec((tile, d), lambda p, t: (t, 0)), any_, any_, any_],
        out_specs=[pl.BlockSpec((tile, width), lambda p, t: (t, p))] * 3
        + [pl.BlockSpec((d, tile), lambda p, t: (0, jnp.where(p == 0, t, tiles - 1))), any_, any_, any_],
        scratch_shapes=[pltpu.VMEM((d, f), BF)] * 2 + gather_sems(2 * parts + 3),
        compiler_params=pltpu.CompilerParams(
            collective_id=0, has_side_effects=True, vmem_limit_bytes=LIMIT, dimension_semantics=("arbitrary", "arbitrary")
        ),
        cost_estimate=pl.CostEstimate(flops=4 * tokens * d * f, bytes_accessed=110_000_000, transcendentals=tokens * f),
        name="gate_up",
    )(h, wg, wu, wd)


def down_kernel(tiles, hid_ref, h_ref, w_ref, wd_ref, h1_ref, wd1_ref, send, recv, local):
    step = pl.program_id(0)
    place = Place()
    sems = lambda j: (send.at[j], recv.at[j], local.at[j])
    rows = wd_ref.shape[1]
    down = Gather(place, wd_ref.at[1], wd1_ref, (0, (rows // 2 // 16 + 1) // 2 * 16, rows // 2 - (rows // 2 // 16 + 1) // 2 * 16), sems(0))
    on(step == 0, place.barrier, down.start)
    on(step == tiles // 2 + 1, down.second)
    on(step == tiles // 2 + 2, down.third)
    h1_ref[...] = h_ref[...] + dot(hid_ref[...], w_ref[...]).astype(BF)
    on(step == tiles - 1, down.fourth, down.finish)


def down(hid, h, w, wd):
    tokens, d = h.shape
    f = hid.shape[1]
    tile = 512
    any_ = pl.BlockSpec(memory_space=pl.ANY)
    return pl.pallas_call(
        functools.partial(down_kernel, tokens // tile),
        grid=(tokens // tile,),
        out_shape=[jax.ShapeDtypeStruct((tokens, d), BF), jax.ShapeDtypeStruct((f, d), BF)],
        in_specs=[
            pl.BlockSpec((tile, f), lambda t: (t, 0)),
            pl.BlockSpec((tile, d), lambda t: (t, 0)),
            pl.BlockSpec((f, d), lambda t: (0, 0), pipeline_mode=pl.Buffered(1)),
            any_,
        ],
        out_specs=[pl.BlockSpec((tile, d), lambda t: (t, 0)), any_],
        scratch_shapes=gather_sems(1),
        compiler_params=pltpu.CompilerParams(collective_id=1, has_side_effects=True, vmem_limit_bytes=LIMIT, dimension_semantics=("arbitrary",)),
        cost_estimate=pl.CostEstimate(flops=2 * tokens * d * f, bytes_accessed=37_000_000, transcendentals=0),
        name="down",
    )(hid, h, w, wd)


def last_kernel(h_ref, dy_ref, wg_ref, wu_ref, wd_ref, hid_ref, dg_ref, du_ref, at_ref, dyt_ref, dh_ref, dht_ref):
    h = wide(h_ref[...])
    scale = scale_of(h)
    a = (h * scale).astype(BF)
    dy = dy_ref[...]
    at_ref[...] = a.T
    dyt_ref[...] = dy.T
    f = wg_ref.shape[1]
    by_a = jnp.zeros(h.shape, F32)
    for n in range(0, f, 768):
        for k in range(n, n + 768, 256):
            where = slice(k, k + 256)
            g = dot(a, wg_ref[:, where])
            u = dot(a, wu_ref[:, where])
            back = wide(dot(dy, wd_ref[where, :], ((1,), (1,))).astype(BF))
            s = sigmoid(g)
            silu = g * s
            hid_ref[:, where] = (silu * u).astype(BF)
            du_ref[:, where] = (back * silu).astype(BF)
            dg_ref[:, where] = (back * u * (s * (1.0 + g * (1.0 - s)))).astype(BF)
        where = slice(n, n + 768)
        by_a += dot(dg_ref[:, where], wg_ref[:, where], ((1,), (1,))) + dot(du_ref[:, where], wu_ref[:, where], ((1,), (1,)))
    by_a = wide(by_a.astype(BF))
    mean = jnp.mean(by_a * h, -1, keepdims=True)
    by_h = (by_a * scale - h * (scale * scale * scale * mean)).astype(BF)
    by_h = dy + by_h
    dh_ref[...] = by_h
    dht_ref[...] = by_h.T


def last_layer(h, dy, wg, wu, wd):
    tokens, d = h.shape
    f = wg.shape[1]
    tile = 512
    rows = lambda n: pl.BlockSpec((tile, n), lambda t: (t, 0))
    columns = pl.BlockSpec((d, tile), lambda t: (0, t))
    fixed = lambda m, n: pl.BlockSpec((m, n), lambda t: (0, 0), pipeline_mode=pl.Buffered(1))
    shape = lambda *s: jax.ShapeDtypeStruct(s, BF)
    return pl.pallas_call(
        last_kernel,
        grid=(tokens // tile,),
        out_shape=[shape(tokens, f)] * 3 + [shape(d, tokens)] * 2 + [shape(tokens, d), shape(d, tokens)],
        in_specs=[rows(d), rows(d), fixed(d, f), fixed(d, f), fixed(f, d)],
        out_specs=[rows(f)] * 3 + [columns] * 2 + [rows(d), columns],
        compiler_params=pltpu.CompilerParams(vmem_limit_bytes=LIMIT, dimension_semantics=("arbitrary",)),
        cost_estimate=pl.CostEstimate(flops=10 * tokens * d * f, bytes_accessed=110_000_000, transcendentals=tokens * f),
        name="last_layer",
    )(h, dy, wg, wu, wd)


def back_kernel(dh_ref, g_ref, u_ref, wd_ref, dg_ref, du_ref):
    dh = dh_ref[...]
    for k in range(0, g_ref.shape[1], 256):
        where = slice(k, k + 256)
        back = wide(dot(dh, wd_ref[where, :], ((1,), (1,))).astype(BF))
        g, u = g_ref[:, where], u_ref[:, where]
        s = sigmoid(g)
        du_ref[:, where] = (back * (g * s)).astype(BF)
        dg_ref[:, where] = (back * u * (s * (1.0 + g * (1.0 - s)))).astype(BF)


def back_to_hidden(dh, g, u, wd):
    tokens, d = dh.shape
    f = g.shape[1]
    tile = 512
    rows = lambda n: pl.BlockSpec((tile, n), lambda t: (t, 0))
    return pl.pallas_call(
        back_kernel,
        grid=(tokens // tile,),
        out_shape=[jax.ShapeDtypeStruct((tokens, f), BF)] * 2,
        in_specs=[rows(d), rows(f), rows(f), pl.BlockSpec((f, d), lambda t: (0, 0), pipeline_mode=pl.Buffered(1))],
        out_specs=[rows(f)] * 2,
        compiler_params=pltpu.CompilerParams(vmem_limit_bytes=LIMIT, dimension_semantics=("arbitrary",)),
        cost_estimate=pl.CostEstimate(flops=2 * tokens * d * f, bytes_accessed=125_000_000, transcendentals=tokens * f),
        name="back_to_hidden",
    )(dh, g, u, wd)


class Sum:
    COPIES = 7

    def __init__(self, place, store, out, squares, columns, x_first, send, recv):
        self.p, self.out, self.squares, self.x_first = place, out, squares, x_first
        self.term, self.rc, self.sx, self.rx, self.sy, self.ry, self.sz, self.rz = store
        self.rows = self.term.shape[0] // 8
        self.c0, self.width = columns
        self.cols = pl.ds(self.c0, self.width)
        self.send, self.recv = send, recv
        s = place.s
        self.x, self.y, self.core = s // 4, (s // 2) % 2, s % 2

    def chip(self, near, far):
        return near * 2 + far if self.x_first else far * 2 + near

    def block(self, chip, core):
        return pl.ds(pl.multiple_of((chip * 2 + core) * self.rows, 16), self.rows)

    def copy(self, k):
        core, xn, yn, zn = self.p.neighbours()
        first, second = (xn, yn) if self.x_first else (yn, xn)
        if k < 4:
            source, target, device = self.term.at[self.block(k, 1 - self.core), self.cols], self.rc.at[k, :, self.cols], core
        elif k == 4:
            source, target, device = self.sx.at[:, :, self.cols], self.rx.at[:, :, self.cols], first
        elif k == 5:
            source, target, device = self.sy.at[:, self.cols], self.ry.at[:, self.cols], second
        else:
            source, target, device = self.sz.at[:, self.cols], self.rz.at[:, self.cols], zn
        return pltpu.make_async_remote_copy(
            src_ref=source, dst_ref=target, send_sem=self.send.at[k], recv_sem=self.recv.at[k], device_id=device, device_id_type=MESH
        )

    def mine(self, chip, r):
        start = pl.multiple_of((chip * 2 + self.core) * self.rows + r * 16, 16)
        return wide(self.term[pl.ds(start, 16), self.cols]) + wide(self.rc[chip, pl.ds(pl.multiple_of(r * 16, 16), 16), self.cols])

    def each(self, body):
        def go(r, carry):
            body(r, pl.ds(pl.multiple_of(r * 16, 16), 16))
            return carry

        lax.fori_loop(0, self.rows // 16, go, 0)

    def stage0(self):
        for k in range(4):
            self.copy(k).start()

    def stage1(self):
        for k in range(4):
            self.copy(k).wait_recv()
        near = (1 - self.x) if self.x_first else (1 - self.y)

        def body(r, rows):
            for far in range(2):
                self.sx[far, rows, self.cols] = self.mine(self.chip(near, far), r).astype(BF)

        self.each(body)
        self.copy(4).start()

    def stage2(self):
        self.copy(4).wait_recv()
        near, far = (self.x, 1 - self.y) if self.x_first else (self.y, 1 - self.x)

        def body(r, rows):
            self.sy[rows, self.cols] = (self.mine(self.chip(near, far), r) + wide(self.rx[far, rows, self.cols])).astype(BF)

        self.each(body)
        self.copy(5).start()

    def stage3(self):
        self.copy(5).wait_recv()
        for k in range(4):
            self.copy(k).wait_send()
        near, far = (self.x, self.y) if self.x_first else (self.y, self.x)

        def body(r, rows):
            total = self.mine(self.chip(near, far), r) + wide(self.rx[far, rows, self.cols]) + wide(self.ry[rows, self.cols])
            self.sz[rows, self.cols] = total.astype(BF)

        self.each(body)
        self.copy(6).start()

    def stage4(self):
        self.copy(6).wait_recv()

        def body(r, rows):
            total = (wide(self.sz[rows, self.cols]) + wide(self.rz[rows, self.cols])).astype(BF)
            self.out[rows, self.cols] = total
            square = wide(total) * wide(total)
            square = square[:8] + square[8:]
            part = square[:, :LANES]
            for k in range(LANES, self.width, LANES):
                part = part + square[:, k : k + LANES]
            self.squares[...] += part

        self.each(body)
        for k in range(4, self.COPIES):
            self.copy(k).wait_send()


TILE = 256


def gradients_kernel(phases, pieces, tiles, *refs):
    lefts, rights = refs[:4], refs[4:10]
    outs, total_ref = refs[10:16], refs[16]
    left, right, l_sem, r_sem, *rest = refs[17:]
    stores = [rest[8 * i : 8 * i + 8] for i in range(3)]
    squares, parts, send, recv, psend, precv, free = rest[24:]
    place = Place()
    s, z = place.s, place.z
    barrier = pltpu.get_barrier_semaphore()
    peers = [(s + k) % 8 for k in range(1, 8)]
    for peer in peers:
        pl.semaphore_signal(barrier, inc=1, device_id={"s": peer}, device_id_type=MESH)
    pl.semaphore_signal(barrier, inc=1, device_id={"r": 1 - z}, device_id_type=MESH)
    pl.semaphore_wait(barrier, 8)

    sums = [Sum(place, stores[p["store"]], outs[p["phase"]], squares, p["columns"], p["x_first"], send.at[q], recv.at[q]) for q, p in enumerate(pieces)]
    neighbours = place.neighbours()

    def give(pair):
        for d, device in enumerate(neighbours):
            pl.semaphore_signal(free.at[pair, d], inc=1, device_id=device, device_id_type=MESH)

    def take(pair):
        for d in range(4):
            pl.semaphore_wait(free.at[pair, d], 1)

    def load_left(k):
        return pltpu.make_async_copy(lefts[k], left.at[k % 2], l_sem.at[k % 2])

    def load_right(phase, i, slot):
        cols = pl.ds(pl.multiple_of(i * TILE, TILE), TILE)
        return pltpu.make_async_copy(rights[phase].at[:, cols], right.at[slot], r_sem.at[slot])

    squares[...] = jnp.zeros_like(squares)
    load_left(0).start()
    load_right(0, 0, 0).start()
    load_left(1).start()
    load_right(0, 1, 1).start()
    at = {}
    for q, p in enumerate(pieces):
        for stage, step in enumerate(p["steps"]):
            at.setdefault(step, []).append((q, stage))

    def run(q, stage):
        p = pieces[q]
        if stage == 0 and p["take"] is not None:
            take(p["take"])
        getattr(sums[q], f"stage{stage}")()
        if stage == 4 and p["give"] is not None:
            give(p["give"])

    slots = 2
    for n, (which, turned, store, loads) in enumerate(phases):
        if n == 0 or phases[n - 1][0] != which:
            load_left(which).wait()
        if loads is not None:
            load_left(loads).start()
        term = stores[store][0]

        def tile(i, carry, n=n, which=which, turned=turned, term=term):
            for k in range(tiles):
                if n * tiles + k in at:
                    on(i == k, *[functools.partial(run, q, stage) for q, stage in at[n * tiles + k]])
            slot = (n * tiles + i) % slots
            load_right(n, i, slot).wait()
            total = dot(left[which % 2], right[slot])
            where = pl.ds(pl.multiple_of(i * TILE, TILE), TILE)
            if turned:
                term[where, :] = total.T.astype(BF)
            else:
                term[:, where] = total.astype(BF)

            @pl.when(i + slots < tiles)
            def _():
                load_right(n, i + slots, slot).start()

            if n + 1 < len(phases):

                @pl.when(i + slots >= tiles)
                def _():
                    load_right(n + 1, i + slots - tiles, slot).start()

            return carry

        lax.fori_loop(0, tiles, tile, 0)

    for step in sorted(at):
        if step >= len(phases) * tiles:
            for q, stage in at[step]:
                run(q, stage)

    def share(k):
        return pltpu.make_async_remote_copy(
            src_ref=squares,
            dst_ref=parts.at[s],
            send_sem=psend.at[k - 1],
            recv_sem=precv.at[k - 1],
            device_id={"s": peers[k - 1]},
            device_id_type=MESH,
        )

    for k in range(1, 8):
        share(k).start()
    parts[s] = squares[...]
    for k in range(1, 8):
        share(k).wait()
    total = parts[0]
    for k in range(1, 8):
        total = total + parts[k]
    total_ref[...] = total


def gradients(lefts, rights):
    d, tokens = lefts[0].shape
    f = rights[0].shape[1]
    tiles = f // TILE
    phases = [(0, True, 2, None), (1, False, 0, 2), (1, False, 1, None), (2, True, 2, 3), (3, False, 0, None), (3, False, 1, None)]
    gives, takes = {0: 2, 1: 0, 2: 1}, {3: 2, 4: 0, 5: 1}
    pieces = []
    for phase, (_, turned, store_of, _) in enumerate(phases):
        final = phase == len(phases) - 1
        columns = d if turned else f
        cuts = [0, 3 * TILE, 6 * TILE, columns - 3 * LANES, columns] if final else [0, -(-columns // 2 // LANES) * LANES, columns]
        gaps = (0, 2, 6, 9, 12) if final else (0, 2, 8, 12, 18)
        for n, (a, b) in enumerate(zip(cuts, cuts[1:])):
            ready = phase * tiles + (tiles if turned else -(-b // TILE))
            pieces.append(
                dict(
                    phase=phase,
                    store=store_of,
                    columns=(a, b - a),
                    x_first=n % 2 == 0,
                    steps=[ready + gap for gap in gaps],
                    take=takes.get(phase) if a == 0 else None,
                    give=gives.get(phase) if b == columns else None,
                )
            )
    shape = lambda *s: pltpu.VMEM(s, BF)

    def store(rows, columns):
        return [
            shape(8 * rows, columns),
            shape(4, rows, columns),
            shape(2, rows, columns),
            shape(2, rows, columns),
            *[shape(rows, columns)] * 4,
        ]

    any_ = pl.BlockSpec(memory_space=pl.ANY)
    vmem = pl.BlockSpec(memory_space=pltpu.VMEM)
    blocks = [jax.ShapeDtypeStruct((f // 8, d) if turned else (d // 8, f), BF) for _, turned, _, _ in phases]
    return pl.pallas_call(
        functools.partial(gradients_kernel, phases, pieces, tiles),
        out_shape=blocks + [jax.ShapeDtypeStruct((8, LANES), F32)],
        in_specs=[any_] * 10,
        out_specs=[vmem] * 7,
        scratch_shapes=[
            pltpu.VMEM((2, d, tokens), BF),
            pltpu.VMEM((2, tokens, TILE), BF),
            pltpu.SemaphoreType.DMA((2,)),
            pltpu.SemaphoreType.DMA((2,)),
            *store(d // 8, f),
            *store(d // 8, f),
            *store(f // 8, d),
            pltpu.VMEM((8, LANES), F32),
            pltpu.VMEM((8, 8, LANES), F32),
            pltpu.SemaphoreType.DMA((len(pieces), Sum.COPIES)),
            pltpu.SemaphoreType.DMA((len(pieces), Sum.COPIES)),
            pltpu.SemaphoreType.DMA((7,)),
            pltpu.SemaphoreType.DMA((7,)),
            pltpu.SemaphoreType.REGULAR((3, 4)),
        ],
        compiler_params=pltpu.CompilerParams(collective_id=2, has_side_effects=True, vmem_limit_bytes=67_043_328),
        cost_estimate=pl.CostEstimate(flops=12 * tokens * d * f, bytes_accessed=150_000_000, transcendentals=0),
        name="gradients",
    )(*lefts, *rights)


def adamw(w, m, v, g):
    m = 0.9 * m + 0.1 * g
    v = 0.95 * v + 0.05 * g * g
    step = m * lax.rsqrt(v + 1e-8) + 0.1 * w
    return (w - 0.02 * step).astype(jnp.bfloat16), m, v


def solution(mesh):
    def step(x, dy, *arrays):
        weights, m, v = (arrays[i : i + 3] for i in (0, 3, 6))
        wg, wu, wd = weights
        x, dy = x[0], dy[0]
        g, u, hid0, at0, wd0, wg1, wu1 = gate_up(x, wg, wu, wd)
        h, wd1 = down(hid0, x, wd0, wd)
        hid1, dg1, du1, at1, dyt, dh, dht = last_layer(h, dy, wg1, wu1, wd1)
        dg0, du0 = back_to_hidden(dh, g, u, wd0)
        d1, g1, u1, d0, g0, u0, squares = gradients((dyt, at1, dht, at0), (hid1, dg1, du1, hid0, dg0, du0))
        own = [jnp.stack(pair).astype(F32) for pair in ((g0, g1), (u0, u1), (d0, d1))]
        count = lax.psum(1, "s") * sum(g.size for g in own)
        factor = jnp.minimum(1.0, 0.5 * lax.rsqrt(jnp.sum(squares) / count + 1e-30))
        new = [adamw(w.astype(F32), m, v, g * factor) for w, m, v, g in zip(weights, m, v, own, strict=True)]
        return tuple(one[which] for which in range(3) for one in new)

    states, cut = P(("rep", "r", "s"), None, None), P(None, "s", None)
    return jax.shard_map(
        step,
        mesh=mesh,
        in_specs=(states, states) + (cut,) * 9,
        out_specs=(P("rep", "s", None),) * 9,
        check_vma=False,
    )
```

```python
import functools

import jax
import jax.numpy as jnp
from jax import lax
from jax.experimental import pallas as pl
from jax.experimental.pallas import tpu as pltpu
from jax.sharding import PartitionSpec as P

NAMES = ("w_gate", "w_up", "w_down")
MESH = pl.DeviceIdType.MESH
BF, F32 = jnp.bfloat16, jnp.float32
LIMIT = 60 * 1024 * 1024
LANES = 128


def wide(a):
    return a.astype(F32)


def dot(a, b, contract=((1,), (0,))):
    return lax.dot_general(a, b, (contract, ((), ())), preferred_element_type=F32)


def scale_of(h):
    return lax.rsqrt(jnp.mean(h * h, -1, keepdims=True) + 1e-6)


class Place:
    def __init__(self):
        s = lax.axis_index("s")
        x, y, core = s // 4, (s // 2) % 2, s % 2
        at = lambda x, y, core: x * 4 + y * 2 + core
        self.s, self.z = s, lax.axis_index("r")
        self.other, self.xn, self.yn, self.diagonal = at(x, y, 1 - core), at(1 - x, y, core), at(x, 1 - y, core), at(1 - x, 1 - y, core)

    def neighbours(self):
        return ({"s": self.other}, {"s": self.xn}, {"s": self.yn}, {"r": 1 - self.z}, {"s": self.diagonal})

    def barrier(self):
        barrier = pltpu.get_barrier_semaphore()
        for device in self.neighbours():
            pl.semaphore_signal(barrier, inc=1, device_id=device, device_id_type=MESH)
        pl.semaphore_wait(barrier, len(self.neighbours()))


TRANSFERS = 13


class Gather:
    def __init__(self, place, block, whole, axis, sems):
        self.p, self.block, self.whole, self.axis = place, block, whole, axis
        self.rows = block.shape[0]
        size = block.shape[axis]
        grain = LANES if axis else 16
        self.half = size // 2
        self.first = (self.half // grain + 1) // 2 * grain
        self.send, self.recv, self.local = sems
        core, xn, yn, zn, diagonal = place.neighbours()
        z, inner = place.z, size - self.first
        most, half = (z * self.first, inner), (z * self.half, self.half)
        edge, edge2 = (z * inner, self.first), ((1 - z) * inner, self.first)
        own, x, y, d = place.s, place.xn, place.yn, place.diagonal
        half2 = ((1 - z) * self.half, self.half)
        every = [(own, (0, size), core), (own, most, xn), (own, most, yn), (own, half, diagonal)]
        every += [(x, most, core), (y, most, core), (d, half, core), (x, edge, zn), (y, edge, zn), (d, half, zn)]
        every += [(x, edge2, core), (y, edge2, core), (d, half2, core)]
        self.every = every

    def part(self, ref, s, offset, size):
        start = 0 if s is None else pl.multiple_of(s * self.rows, 16)
        if self.axis:
            return ref.at[pl.ds(start, self.rows), pl.ds(pl.multiple_of(offset, LANES), size)]
        return ref.at[pl.ds(start + pl.multiple_of(offset, 16), size)]

    def copy(self, k):
        s, (offset, size), device = self.every[k]
        target = self.part(self.whole, s, offset, size)
        source = self.part(self.block, None, offset, size) if s is self.p.s else target
        return pltpu.make_async_remote_copy(
            src_ref=source, dst_ref=target, send_sem=self.send.at[k], recv_sem=self.recv.at[k], device_id=device, device_id_type=MESH
        )

    def keep(self):
        return pltpu.make_async_copy(self.block, self.whole.at[pl.ds(pl.multiple_of(self.p.s * self.rows, 16), self.rows)], self.local)

    def start(self):
        for k in (1, 2, 3, 0):
            self.copy(k).start()
        self.keep().start()

    def second(self):
        for k in (1, 2, 3):
            self.copy(k).wait_recv()
        for k in (7, 8, 9, 4, 5, 6):
            self.copy(k).start()

    def third(self):
        for k in (7, 8, 9):
            self.copy(k).wait_recv()
            self.copy(k + 3).start()

    def finish(self):
        for k in (0, 4, 5, 6, 10, 11, 12):
            self.copy(k).wait_recv()
        for k in range(TRANSFERS):
            self.copy(k).wait_send()
        self.keep().wait()


def gather_sems(jobs):
    return [pltpu.SemaphoreType.DMA((jobs, TRANSFERS)), pltpu.SemaphoreType.DMA((jobs, TRANSFERS)), pltpu.SemaphoreType.DMA((jobs,))]


def on(step, *actions):
    @pl.when(step)
    def _():
        for action in actions:
            action()


def sigmoid(x):
    return 0.5 * jnp.tanh(0.5 * x) + 0.5


def gate_up_kernel(parts, tiles, h_ref, wg_ref, wu_ref, wd_ref, g_ref, u_ref, hid_ref, at_ref, wd0_ref, wg1_ref, wu1_ref, wg, wu, send, recv, local):
    part, tile = pl.program_id(0), pl.program_id(1)
    step = part * tiles + tile
    place = Place()
    width = g_ref.shape[1]
    f = wg_ref.shape[2]
    middle = (f // LANES + 2) // 4 * 2 * LANES
    ranges = [(own.at[0], whole, pl.ds(n * width, width), 1) for n in range(parts) for own, whole in ((wg_ref, wg), (wu_ref, wu))]
    ranges += [(wd_ref.at[0], wd0_ref, pl.ds(0, wd_ref.shape[2]), 0), (wg_ref.at[1], wg1_ref, pl.ds(0, f), 1)]
    ranges += [(wu_ref.at[1], wu1_ref, cols, 1) for cols in (pl.ds(0, middle), pl.ds(middle, f - middle))]
    jobs = [
        Gather(place, own.at[:, cols], whole.at[:, cols], axis, (send.at[k], recv.at[k], local.at[k])) for k, (own, whole, cols, axis) in enumerate(ranges)
    ]
    b0, b1, b2, (down, gate1), up1 = [jobs[k : k + 2] for k in range(0, len(jobs), 2)]
    both = lambda pair, *stages: [getattr(job, stage) for stage in stages for job in pair]
    last = parts * tiles - 1

    on(step == 0, place.barrier, *both(b0, "start"), *both(b1, "start"), *both(b0, "second", "third", "finish"), *both(b2, "start"))
    on(step == 1, *both(b1, "second"), down.start)
    on(step == 5, *both(b2, "second"), gate1.start)
    on(step == 6, *both(b1, "third"))
    on(step == tiles, *both(b1, "finish"))
    on(step == 10, *both(b2, "third"), down.second)
    on(step == 11, *both(up1, "start"))
    on(step == 2 * tiles, *both(b2, "finish"), down.third, gate1.second)
    on(step == 18, down.finish)
    on(step == 20, up1[0].second)
    on(step == 22, gate1.third)
    on(step == last, gate1.finish, up1[1].second)

    h = wide(h_ref[...])
    a = (h * scale_of(h)).astype(BF)

    @pl.when(part == 0)
    def _():
        at_ref[...] = a.T

    for n in range(0, width, 256):
        where = pl.ds(pl.multiple_of(part * width + n, LANES), 256)
        g = dot(a, wg[:, where])
        u = dot(a, wu[:, where])
        g_ref[:, n : n + 256] = g
        u_ref[:, n : n + 256] = u
        hid_ref[:, n : n + 256] = (g * sigmoid(g) * u).astype(BF)

    on(step == last, *both(up1, "third", "finish"))


def gate_up(h, wg, wu, wd):
    tokens, d = h.shape
    _, rows, f = wg.shape
    parts, tile = 3, 512
    width, tiles = f // parts, tokens // tile
    group = d // rows
    any_ = pl.BlockSpec(memory_space=pl.ANY)
    return pl.pallas_call(
        functools.partial(gate_up_kernel, parts, tiles),
        grid=(parts, tiles),
        out_shape=[
            jax.ShapeDtypeStruct((tokens, f), F32),
            jax.ShapeDtypeStruct((tokens, f), F32),
            jax.ShapeDtypeStruct((tokens, f), BF),
            jax.ShapeDtypeStruct((d, tokens), BF),
            jax.ShapeDtypeStruct((wd.shape[1] * group, d), BF),
            jax.ShapeDtypeStruct((d, f), BF),
            jax.ShapeDtypeStruct((d, f), BF),
        ],
        in_specs=[pl.BlockSpec((tile, d), lambda p, t: (t, 0)), any_, any_, any_],
        out_specs=[pl.BlockSpec((tile, width), lambda p, t: (t, p))] * 3
        + [pl.BlockSpec((d, tile), lambda p, t: (0, jnp.where(p == 0, t, tiles - 1))), any_, any_, any_],
        scratch_shapes=[pltpu.VMEM((d, f), BF)] * 2 + gather_sems(2 * parts + 4),
        compiler_params=pltpu.CompilerParams(
            collective_id=0, has_side_effects=True, vmem_limit_bytes=LIMIT, dimension_semantics=("arbitrary", "arbitrary")
        ),
        cost_estimate=pl.CostEstimate(flops=4 * tokens * d * f, bytes_accessed=110_000_000, transcendentals=tokens * f),
        name="gate_up",
    )(h, wg, wu, wd)


def down_kernel(tiles, hid_ref, h_ref, w_ref, wd_ref, h1_ref, wd1_ref, send, recv, local):
    step = pl.program_id(0)
    place = Place()
    d = wd_ref.shape[2]
    middle = (d // LANES + 1) // 2 * LANES
    jobs = [
        Gather(place, wd_ref.at[1, :, cols], wd1_ref.at[:, cols], 0, (send.at[k], recv.at[k], local.at[k]))
        for k, cols in enumerate((pl.ds(0, middle), pl.ds(middle, d - middle)))
    ]
    on(step == 0, place.barrier, *[job.start for job in jobs])
    on(step == tiles - 3, jobs[0].second)
    on(step == tiles - 1, jobs[1].second)
    h1_ref[...] = h_ref[...] + dot(hid_ref[...], w_ref[...]).astype(BF)
    on(step == tiles - 1, *[job.third for job in jobs], *[job.finish for job in jobs])


def down(hid, h, w, wd):
    tokens, d = h.shape
    f = hid.shape[1]
    tile = 512
    any_ = pl.BlockSpec(memory_space=pl.ANY)
    return pl.pallas_call(
        functools.partial(down_kernel, tokens // tile),
        grid=(tokens // tile,),
        out_shape=[jax.ShapeDtypeStruct((tokens, d), BF), jax.ShapeDtypeStruct((f, d), BF)],
        in_specs=[
            pl.BlockSpec((tile, f), lambda t: (t, 0)),
            pl.BlockSpec((tile, d), lambda t: (t, 0)),
            pl.BlockSpec((f, d), lambda t: (0, 0), pipeline_mode=pl.Buffered(1)),
            any_,
        ],
        out_specs=[pl.BlockSpec((tile, d), lambda t: (t, 0)), any_],
        scratch_shapes=gather_sems(2),
        compiler_params=pltpu.CompilerParams(collective_id=1, has_side_effects=True, vmem_limit_bytes=LIMIT, dimension_semantics=("arbitrary",)),
        cost_estimate=pl.CostEstimate(flops=2 * tokens * d * f, bytes_accessed=37_000_000, transcendentals=0),
        name="down",
    )(hid, h, w, wd)


def last_kernel(h_ref, dy_ref, wg_ref, wu_ref, wd_ref, hid_ref, dg_ref, du_ref, at_ref, dyt_ref, dh_ref, dht_ref):
    h = wide(h_ref[...])
    scale = scale_of(h)
    a = (h * scale).astype(BF)
    dy = dy_ref[...]
    at_ref[...] = a.T
    dyt_ref[...] = dy.T
    f = wg_ref.shape[1]
    by_a = jnp.zeros(h.shape, F32)
    for n in range(0, f, 768):
        for k in range(n, n + 768, 256):
            where = slice(k, k + 256)
            g = dot(a, wg_ref[:, where])
            u = dot(a, wu_ref[:, where])
            back = wide(dot(dy, wd_ref[where, :], ((1,), (1,))).astype(BF))
            s = sigmoid(g)
            silu = g * s
            hid_ref[:, where] = (silu * u).astype(BF)
            du_ref[:, where] = (back * silu).astype(BF)
            dg_ref[:, where] = (back * u * (s * (1.0 + g * (1.0 - s)))).astype(BF)
        where = slice(n, n + 768)
        by_a += dot(dg_ref[:, where], wg_ref[:, where], ((1,), (1,))) + dot(du_ref[:, where], wu_ref[:, where], ((1,), (1,)))
    by_a = wide(by_a.astype(BF))
    mean = jnp.mean(by_a * h, -1, keepdims=True)
    by_h = (by_a * scale - h * (scale * scale * scale * mean)).astype(BF)
    by_h = dy + by_h
    dh_ref[...] = by_h
    dht_ref[...] = by_h.T


def last_layer(h, dy, wg, wu, wd):
    tokens, d = h.shape
    f = wg.shape[1]
    tile = 512
    rows = lambda n: pl.BlockSpec((tile, n), lambda t: (t, 0))
    columns = pl.BlockSpec((d, tile), lambda t: (0, t))
    fixed = lambda m, n: pl.BlockSpec((m, n), lambda t: (0, 0), pipeline_mode=pl.Buffered(1))
    shape = lambda *s: jax.ShapeDtypeStruct(s, BF)
    return pl.pallas_call(
        last_kernel,
        grid=(tokens // tile,),
        out_shape=[shape(tokens, f)] * 3 + [shape(d, tokens)] * 2 + [shape(tokens, d), shape(d, tokens)],
        in_specs=[rows(d), rows(d), fixed(d, f), fixed(d, f), fixed(f, d)],
        out_specs=[rows(f)] * 3 + [columns] * 2 + [rows(d), columns],
        compiler_params=pltpu.CompilerParams(vmem_limit_bytes=LIMIT, dimension_semantics=("arbitrary",)),
        cost_estimate=pl.CostEstimate(flops=10 * tokens * d * f, bytes_accessed=110_000_000, transcendentals=tokens * f),
        name="last_layer",
    )(h, dy, wg, wu, wd)


def back_kernel(dh_ref, g_ref, u_ref, wd_ref, dg_ref, du_ref):
    dh = dh_ref[...]
    for k in range(0, g_ref.shape[1], 256):
        where = slice(k, k + 256)
        back = wide(dot(dh, wd_ref[where, :], ((1,), (1,))).astype(BF))
        g, u = g_ref[:, where], u_ref[:, where]
        s = sigmoid(g)
        du_ref[:, where] = (back * (g * s)).astype(BF)
        dg_ref[:, where] = (back * u * (s * (1.0 + g * (1.0 - s)))).astype(BF)


def back_to_hidden(dh, g, u, wd):
    tokens, d = dh.shape
    f = g.shape[1]
    tile = 512
    rows = lambda n: pl.BlockSpec((tile, n), lambda t: (t, 0))
    return pl.pallas_call(
        back_kernel,
        grid=(tokens // tile,),
        out_shape=[jax.ShapeDtypeStruct((tokens, f), BF)] * 2,
        in_specs=[rows(d), rows(f), rows(f), pl.BlockSpec((f, d), lambda t: (0, 0), pipeline_mode=pl.Buffered(1))],
        out_specs=[rows(f)] * 2,
        compiler_params=pltpu.CompilerParams(vmem_limit_bytes=LIMIT, dimension_semantics=("arbitrary",)),
        cost_estimate=pl.CostEstimate(flops=2 * tokens * d * f, bytes_accessed=125_000_000, transcendentals=tokens * f),
        name="back_to_hidden",
    )(dh, g, u, wd)


class Sum:
    COPIES = 7

    def __init__(self, place, store, out, squares, columns, x_first, send, recv):
        self.p, self.out, self.squares, self.x_first = place, out, squares, x_first
        self.term, self.rc, self.sx, self.rx, self.sy, self.ry, self.sz, self.rz = store
        self.rows = self.term.shape[0] // 8
        self.c0, self.width = columns
        self.cols = pl.ds(self.c0, self.width)
        self.send, self.recv = send, recv
        s = place.s
        self.x, self.y, self.core = s // 4, (s // 2) % 2, s % 2

    def chip(self, near, far):
        return near * 2 + far if self.x_first else far * 2 + near

    def block(self, chip, core):
        return pl.ds(pl.multiple_of((chip * 2 + core) * self.rows, 16), self.rows)

    def copy(self, k):
        core, xn, yn, zn, _ = self.p.neighbours()
        first, second = (xn, yn) if self.x_first else (yn, xn)
        if k < 4:
            source, target, device = self.term.at[self.block(k, 1 - self.core), self.cols], self.rc.at[k, :, self.cols], core
        elif k == 4:
            source, target, device = self.sx.at[:, :, self.cols], self.rx.at[:, :, self.cols], first
        elif k == 5:
            source, target, device = self.sy.at[:, self.cols], self.ry.at[:, self.cols], second
        else:
            source, target, device = self.sz.at[:, self.cols], self.rz.at[:, self.cols], zn
        return pltpu.make_async_remote_copy(
            src_ref=source, dst_ref=target, send_sem=self.send.at[k], recv_sem=self.recv.at[k], device_id=device, device_id_type=MESH
        )

    def mine(self, chip, r):
        start = pl.multiple_of((chip * 2 + self.core) * self.rows + r * 16, 16)
        return wide(self.term[pl.ds(start, 16), self.cols]) + wide(self.rc[chip, pl.ds(pl.multiple_of(r * 16, 16), 16), self.cols])

    def each(self, body):
        def go(r, carry):
            body(r, pl.ds(pl.multiple_of(r * 16, 16), 16))
            return carry

        lax.fori_loop(0, self.rows // 16, go, 0)

    def stage0(self):
        for k in range(4):
            self.copy(k).start()

    def stage1(self):
        for k in range(4):
            self.copy(k).wait_recv()
        near = (1 - self.x) if self.x_first else (1 - self.y)

        def body(r, rows):
            for far in range(2):
                self.sx[far, rows, self.cols] = self.mine(self.chip(near, far), r).astype(BF)

        self.each(body)
        self.copy(4).start()

    def stage2(self):
        self.copy(4).wait_recv()
        near, far = (self.x, 1 - self.y) if self.x_first else (self.y, 1 - self.x)

        def body(r, rows):
            self.sy[rows, self.cols] = (self.mine(self.chip(near, far), r) + wide(self.rx[far, rows, self.cols])).astype(BF)

        self.each(body)
        self.copy(5).start()

    def stage3(self):
        self.copy(5).wait_recv()
        for k in range(4):
            self.copy(k).wait_send()
        near, far = (self.x, self.y) if self.x_first else (self.y, self.x)

        def body(r, rows):
            total = self.mine(self.chip(near, far), r) + wide(self.rx[far, rows, self.cols]) + wide(self.ry[rows, self.cols])
            self.sz[rows, self.cols] = total.astype(BF)

        self.each(body)
        self.copy(6).start()

    def stage4(self):
        self.copy(6).wait_recv()

        def body(r, rows):
            total = (wide(self.sz[rows, self.cols]) + wide(self.rz[rows, self.cols])).astype(BF)
            self.out[rows, self.cols] = total
            square = wide(total) * wide(total)
            square = square[:8] + square[8:]
            part = square[:, :LANES]
            for k in range(LANES, self.width, LANES):
                part = part + square[:, k : k + LANES]
            self.squares[...] += part

        self.each(body)
        for k in range(4, self.COPIES):
            self.copy(k).wait_send()


TILE = 256


def gradients_kernel(phases, pieces, tiles, *refs):
    lefts, rights = refs[:4], refs[4:10]
    outs, total_ref = refs[10:16], refs[16]
    left, right, l_sem, r_sem, *rest = refs[17:]
    stores = [rest[8 * i : 8 * i + 8] for i in range(3)]
    squares, parts, send, recv, psend, precv, free = rest[24:]
    place = Place()
    s, z = place.s, place.z
    barrier = pltpu.get_barrier_semaphore()
    peers = [(s + k) % 8 for k in range(1, 8)]
    for peer in peers:
        pl.semaphore_signal(barrier, inc=1, device_id={"s": peer}, device_id_type=MESH)
    pl.semaphore_signal(barrier, inc=1, device_id={"r": 1 - z}, device_id_type=MESH)
    pl.semaphore_wait(barrier, 8)

    sums = [Sum(place, stores[p["store"]], outs[p["phase"]], squares, p["columns"], p["x_first"], send.at[q], recv.at[q]) for q, p in enumerate(pieces)]
    neighbours = place.neighbours()[:4]

    def give(pair):
        for d, device in enumerate(neighbours):
            pl.semaphore_signal(free.at[pair, d], inc=1, device_id=device, device_id_type=MESH)

    def take(pair):
        for d in range(4):
            pl.semaphore_wait(free.at[pair, d], 1)

    def load_left(k):
        return pltpu.make_async_copy(lefts[k], left.at[k % 2], l_sem.at[k % 2])

    def load_right(phase, i, slot):
        cols = pl.ds(pl.multiple_of(i * TILE, TILE), TILE)
        return pltpu.make_async_copy(rights[phase].at[:, cols], right.at[slot], r_sem.at[slot])

    squares[...] = jnp.zeros_like(squares)
    load_left(0).start()
    load_right(0, 0, 0).start()
    load_left(1).start()
    load_right(0, 1, 1).start()
    at = {}
    for q, p in enumerate(pieces):
        for stage, step in enumerate(p["steps"]):
            at.setdefault(step, []).append((q, stage))

    def run(q, stage):
        p = pieces[q]
        if stage == 0 and p["take"] is not None:
            take(p["take"])
        getattr(sums[q], f"stage{stage}")()
        if stage == 4 and p["give"] is not None:
            give(p["give"])

    slots = 2
    for n, (which, turned, store, loads) in enumerate(phases):
        if n == 0 or phases[n - 1][0] != which:
            load_left(which).wait()
        if loads is not None:
            load_left(loads).start()
        term = stores[store][0]

        def tile(i, carry, n=n, which=which, turned=turned, term=term):
            for k in range(tiles):
                if n * tiles + k in at:
                    on(i == k, *[functools.partial(run, q, stage) for q, stage in at[n * tiles + k]])
            slot = (n * tiles + i) % slots
            load_right(n, i, slot).wait()
            total = dot(left[which % 2], right[slot])
            where = pl.ds(pl.multiple_of(i * TILE, TILE), TILE)
            if turned:
                term[where, :] = total.T.astype(BF)
            else:
                term[:, where] = total.astype(BF)

            @pl.when(i + slots < tiles)
            def _():
                load_right(n, i + slots, slot).start()

            if n + 1 < len(phases):

                @pl.when(i + slots >= tiles)
                def _():
                    load_right(n + 1, i + slots - tiles, slot).start()

            return carry

        lax.fori_loop(0, tiles, tile, 0)

    for step in sorted(at):
        if step >= len(phases) * tiles:
            for q, stage in at[step]:
                run(q, stage)

    def share(k):
        return pltpu.make_async_remote_copy(
            src_ref=squares,
            dst_ref=parts.at[s],
            send_sem=psend.at[k - 1],
            recv_sem=precv.at[k - 1],
            device_id={"s": peers[k - 1]},
            device_id_type=MESH,
        )

    for k in range(1, 8):
        share(k).start()
    parts[s] = squares[...]
    for k in range(1, 8):
        share(k).wait()
    total = parts[0]
    for k in range(1, 8):
        total = total + parts[k]
    total_ref[...] = total


def gradients(lefts, rights):
    d, tokens = lefts[0].shape
    f = rights[0].shape[1]
    tiles = f // TILE
    phases = [(0, True, 2, None), (1, False, 0, 2), (1, False, 1, None), (2, True, 2, 3), (3, False, 0, None), (3, False, 1, None)]
    gives, takes = {0: 2, 1: 0, 2: 1}, {3: 2, 4: 0, 5: 1}
    pieces = []
    for phase, (_, turned, store_of, _) in enumerate(phases):
        final = phase == len(phases) - 1
        columns = d if turned else f
        cuts = [0, 3 * TILE, 6 * TILE, columns - TILE, columns] if final else [0, -(-columns // 2 // LANES) * LANES, columns]
        gaps = (0, 3, 10, 16, 21) if final else (0, 3, 9, 15, 20)
        for n, (a, b) in enumerate(zip(cuts, cuts[1:])):
            ready = phase * tiles + (tiles if turned else -(-b // TILE))
            pieces.append(
                dict(
                    phase=phase,
                    store=store_of,
                    columns=(a, b - a),
                    x_first=n % 2 == 0,
                    steps=[ready + gap for gap in gaps],
                    take=takes.get(phase) if a == 0 else None,
                    give=gives.get(phase) if b == columns else None,
                )
            )
    shape = lambda *s: pltpu.VMEM(s, BF)

    def store(rows, columns):
        return [
            shape(8 * rows, columns),
            shape(4, rows, columns),
            shape(2, rows, columns),
            shape(2, rows, columns),
            *[shape(rows, columns)] * 4,
        ]

    any_ = pl.BlockSpec(memory_space=pl.ANY)
    vmem = pl.BlockSpec(memory_space=pltpu.VMEM)
    blocks = [jax.ShapeDtypeStruct((f // 8, d) if turned else (d // 8, f), BF) for _, turned, _, _ in phases]
    return pl.pallas_call(
        functools.partial(gradients_kernel, phases, pieces, tiles),
        out_shape=blocks + [jax.ShapeDtypeStruct((8, LANES), F32)],
        in_specs=[any_] * 10,
        out_specs=[vmem] * 7,
        scratch_shapes=[
            pltpu.VMEM((2, d, tokens), BF),
            pltpu.VMEM((2, tokens, TILE), BF),
            pltpu.SemaphoreType.DMA((2,)),
            pltpu.SemaphoreType.DMA((2,)),
            *store(d // 8, f),
            *store(d // 8, f),
            *store(f // 8, d),
            pltpu.VMEM((8, LANES), F32),
            pltpu.VMEM((8, 8, LANES), F32),
            pltpu.SemaphoreType.DMA((len(pieces), Sum.COPIES)),
            pltpu.SemaphoreType.DMA((len(pieces), Sum.COPIES)),
            pltpu.SemaphoreType.DMA((7,)),
            pltpu.SemaphoreType.DMA((7,)),
            pltpu.SemaphoreType.REGULAR((3, 4)),
        ],
        compiler_params=pltpu.CompilerParams(collective_id=2, has_side_effects=True, vmem_limit_bytes=67_043_328),
        cost_estimate=pl.CostEstimate(flops=12 * tokens * d * f, bytes_accessed=150_000_000, transcendentals=0),
        name="gradients",
    )(*lefts, *rights)


def adamw(w, m, v, g):
    m = 0.9 * m + 0.1 * g
    v = 0.95 * v + 0.05 * g * g
    step = m * lax.rsqrt(v + 1e-8) + 0.1 * w
    return (w - 0.02 * step).astype(jnp.bfloat16), m, v


def solution(mesh):
    def step(x, dy, *arrays):
        weights, m, v = (arrays[i : i + 3] for i in (0, 3, 6))
        wg, wu, wd = weights
        x, dy = x[0], dy[0]
        g, u, hid0, at0, wd0, wg1, wu1 = gate_up(x, wg, wu, wd)
        h, wd1 = down(hid0, x, wd0, wd)
        hid1, dg1, du1, at1, dyt, dh, dht = last_layer(h, dy, wg1, wu1, wd1)
        dg0, du0 = back_to_hidden(dh, g, u, wd0)
        d1, g1, u1, d0, g0, u0, squares = gradients((dyt, at1, dht, at0), (hid1, dg1, du1, hid0, dg0, du0))
        own = [jnp.stack(pair).astype(F32) for pair in ((g0, g1), (u0, u1), (d0, d1))]
        count = lax.psum(1, "s") * sum(g.size for g in own)
        factor = jnp.minimum(1.0, 0.5 * lax.rsqrt(jnp.sum(squares) / count + 1e-30))
        new = [adamw(w.astype(F32), m, v, g * factor) for w, m, v, g in zip(weights, m, v, own, strict=True)]
        return tuple(one[which] for which in range(3) for one in new)

    states, cut = P(("rep", "r", "s"), None, None), P(None, "s", None)
    return jax.shard_map(
        step,
        mesh=mesh,
        in_specs=(states, states) + (cut,) * 9,
        out_specs=(P("rep", "s", None),) * 9,
        check_vma=False,
    )
```

```python
import functools

import jax
import jax.numpy as jnp
from jax import lax
from jax.experimental import pallas as pl
from jax.experimental.pallas import tpu as pltpu
from jax.sharding import PartitionSpec as P

NAMES = ("w_gate", "w_up", "w_down")
MESH = pl.DeviceIdType.MESH
BF, F32 = jnp.bfloat16, jnp.float32
LIMIT = 60 * 1024 * 1024
LANES = 128


def wide(a):
    return a.astype(F32)


def dot(a, b, contract=((1,), (0,))):
    return lax.dot_general(a, b, (contract, ((), ())), preferred_element_type=F32)


def scale_of(h):
    return lax.rsqrt(jnp.mean(h * h, -1, keepdims=True) + 1e-6)


class Place:
    def __init__(self):
        s = lax.axis_index("s")
        x, y, core = s // 4, (s // 2) % 2, s % 2
        at = lambda x, y, core: x * 4 + y * 2 + core
        self.s, self.z = s, lax.axis_index("r")
        self.other, self.xn, self.yn, self.diagonal = at(x, y, 1 - core), at(1 - x, y, core), at(x, 1 - y, core), at(1 - x, 1 - y, core)

    def neighbours(self):
        return ({"s": self.other}, {"s": self.xn}, {"s": self.yn}, {"r": 1 - self.z}, {"s": self.diagonal})

    def barrier(self):
        barrier = pltpu.get_barrier_semaphore()
        for device in self.neighbours():
            pl.semaphore_signal(barrier, inc=1, device_id=device, device_id_type=MESH)
        pl.semaphore_wait(barrier, len(self.neighbours()))


TRANSFERS = 13


class Gather:
    def __init__(self, place, block, whole, axis, sems):
        self.p, self.block, self.whole, self.axis = place, block, whole, axis
        self.rows = block.shape[0]
        size = block.shape[axis]
        grain = LANES if axis else 16
        self.half = size // 2
        self.first = (self.half // grain + 1) // 2 * grain
        self.send, self.recv, self.local = sems
        core, xn, yn, zn, diagonal = place.neighbours()
        z, inner = place.z, size - self.first
        most, half = (z * self.first, inner), (z * self.half, self.half)
        edge, edge2 = (z * inner, self.first), ((1 - z) * inner, self.first)
        own, x, y, d = place.s, place.xn, place.yn, place.diagonal
        half2 = ((1 - z) * self.half, self.half)
        every = [(own, (0, size), core), (own, most, xn), (own, most, yn), (own, half, diagonal)]
        every += [(x, most, core), (y, most, core), (d, half, core), (x, edge, zn), (y, edge, zn), (d, half, zn)]
        every += [(x, edge2, core), (y, edge2, core), (d, half2, core)]
        self.every = every

    def part(self, ref, s, offset, size):
        start = 0 if s is None else pl.multiple_of(s * self.rows, 16)
        if self.axis:
            return ref.at[pl.ds(start, self.rows), pl.ds(pl.multiple_of(offset, LANES), size)]
        return ref.at[pl.ds(start + pl.multiple_of(offset, 16), size)]

    def copy(self, k):
        s, (offset, size), device = self.every[k]
        target = self.part(self.whole, s, offset, size)
        source = self.part(self.block, None, offset, size) if s is self.p.s else target
        return pltpu.make_async_remote_copy(
            src_ref=source, dst_ref=target, send_sem=self.send.at[k], recv_sem=self.recv.at[k], device_id=device, device_id_type=MESH
        )

    def keep(self):
        return pltpu.make_async_copy(self.block, self.whole.at[pl.ds(pl.multiple_of(self.p.s * self.rows, 16), self.rows)], self.local)

    def start(self):
        for k in (1, 2, 3, 0):
            self.copy(k).start()
        self.keep().start()

    def second(self):
        for k in (1, 2, 3):
            self.copy(k).wait_recv()
        for k in (7, 8, 9, 4, 5, 6):
            self.copy(k).start()

    def third(self):
        for k in (7, 8, 9):
            self.copy(k).wait_recv()
            self.copy(k + 3).start()

    def finish(self):
        for k in (0, 4, 5, 6, 10, 11, 12):
            self.copy(k).wait_recv()
        for k in range(TRANSFERS):
            self.copy(k).wait_send()
        self.keep().wait()


def gather_sems(jobs):
    return [pltpu.SemaphoreType.DMA((jobs, TRANSFERS)), pltpu.SemaphoreType.DMA((jobs, TRANSFERS)), pltpu.SemaphoreType.DMA((jobs,))]


def on(step, *actions):
    @pl.when(step)
    def _():
        for action in actions:
            action()


def sigmoid(x):
    return 0.5 * jnp.tanh(0.5 * x) + 0.5


def gate_up_kernel(parts, tiles, h_ref, wg_ref, wu_ref, wd_ref, g_ref, u_ref, hid_ref, at_ref, wd0_ref, wg1_ref, wu1_ref, wg, wu, send, recv, local):
    part, tile = pl.program_id(0), pl.program_id(1)
    step = part * tiles + tile
    place = Place()
    width = g_ref.shape[1]
    f = wg_ref.shape[2]
    middle = (f // LANES + 2) // 4 * 2 * LANES
    ranges = [(own.at[0], whole, pl.ds(n * width, width), 1) for n in range(parts) for own, whole in ((wg_ref, wg), (wu_ref, wu))]
    ranges += [(wd_ref.at[0], wd0_ref, pl.ds(0, wd_ref.shape[2]), 0), (wg_ref.at[1], wg1_ref, pl.ds(0, f), 1)]
    ranges += [(wu_ref.at[1], wu1_ref, cols, 1) for cols in (pl.ds(0, middle), pl.ds(middle, f - middle))]
    jobs = [
        Gather(place, own.at[:, cols], whole.at[:, cols], axis, (send.at[k], recv.at[k], local.at[k])) for k, (own, whole, cols, axis) in enumerate(ranges)
    ]
    b0, b1, b2, (down, gate1), up1 = [jobs[k : k + 2] for k in range(0, len(jobs), 2)]
    both = lambda pair, *stages: [getattr(job, stage) for stage in stages for job in pair]
    last = parts * tiles - 1

    on(step == 0, place.barrier, *both(b0, "start"), *both(b1, "start"), *both(b0, "second", "third", "finish"), *both(b2, "start"))
    on(step == 1, *both(b1, "second"), down.start)
    on(step == 5, *both(b2, "second"), gate1.start)
    on(step == 6, *both(b1, "third"))
    on(step == tiles, *both(b1, "finish"))
    on(step == 10, *both(b2, "third"), down.second)
    on(step == 11, *both(up1, "start"))
    on(step == 2 * tiles, *both(b2, "finish"), down.third, gate1.second)
    on(step == 18, down.finish)
    on(step == 20, up1[0].second)
    on(step == 22, gate1.third)
    on(step == last, gate1.finish, up1[1].second)

    h = wide(h_ref[...])
    a = (h * scale_of(h)).astype(BF)

    @pl.when(part == 0)
    def _():
        at_ref[...] = a.T

    for n in range(0, width, 256):
        where = pl.ds(pl.multiple_of(part * width + n, LANES), 256)
        g = dot(a, wg[:, where])
        u = dot(a, wu[:, where])
        g_ref[:, n : n + 256] = g
        u_ref[:, n : n + 256] = u
        hid_ref[:, n : n + 256] = (g * sigmoid(g) * u).astype(BF)

    on(step == last, *both(up1, "third", "finish"))


def gate_up(h, wg, wu, wd):
    tokens, d = h.shape
    _, rows, f = wg.shape
    parts, tile = 3, 512
    width, tiles = f // parts, tokens // tile
    group = d // rows
    any_ = pl.BlockSpec(memory_space=pl.ANY)
    return pl.pallas_call(
        functools.partial(gate_up_kernel, parts, tiles),
        grid=(parts, tiles),
        out_shape=[
            jax.ShapeDtypeStruct((tokens, f), F32),
            jax.ShapeDtypeStruct((tokens, f), F32),
            jax.ShapeDtypeStruct((tokens, f), BF),
            jax.ShapeDtypeStruct((d, tokens), BF),
            jax.ShapeDtypeStruct((wd.shape[1] * group, d), BF),
            jax.ShapeDtypeStruct((d, f), BF),
            jax.ShapeDtypeStruct((d, f), BF),
        ],
        in_specs=[pl.BlockSpec((tile, d), lambda p, t: (t, 0)), any_, any_, any_],
        out_specs=[pl.BlockSpec((tile, width), lambda p, t: (t, p))] * 3
        + [pl.BlockSpec((d, tile), lambda p, t: (0, jnp.where(p == 0, t, tiles - 1))), any_, any_, any_],
        scratch_shapes=[pltpu.VMEM((d, f), BF)] * 2 + gather_sems(2 * parts + 4),
        compiler_params=pltpu.CompilerParams(
            collective_id=0, has_side_effects=True, vmem_limit_bytes=LIMIT, dimension_semantics=("arbitrary", "arbitrary")
        ),
        cost_estimate=pl.CostEstimate(flops=4 * tokens * d * f, bytes_accessed=110_000_000, transcendentals=tokens * f),
        name="gate_up",
    )(h, wg, wu, wd)


def down_kernel(tiles, hid_ref, h_ref, w_ref, wd_ref, h1_ref, wd1_ref, send, recv, local):
    step = pl.program_id(0)
    place = Place()
    d = wd_ref.shape[2]
    middle = (d // LANES + 1) // 2 * LANES
    jobs = [
        Gather(place, wd_ref.at[1, :, cols], wd1_ref.at[:, cols], 0, (send.at[k], recv.at[k], local.at[k]))
        for k, cols in enumerate((pl.ds(0, middle), pl.ds(middle, d - middle)))
    ]
    on(step == 0, place.barrier, *[job.start for job in jobs])
    on(step == tiles - 3, jobs[0].second)
    on(step == tiles - 1, jobs[1].second)
    h1_ref[...] = h_ref[...] + dot(hid_ref[...], w_ref[...]).astype(BF)
    on(step == tiles - 1, *[job.third for job in jobs], *[job.finish for job in jobs])


def down(hid, h, w, wd):
    tokens, d = h.shape
    f = hid.shape[1]
    tile = 512
    any_ = pl.BlockSpec(memory_space=pl.ANY)
    return pl.pallas_call(
        functools.partial(down_kernel, tokens // tile),
        grid=(tokens // tile,),
        out_shape=[jax.ShapeDtypeStruct((tokens, d), BF), jax.ShapeDtypeStruct((f, d), BF)],
        in_specs=[
            pl.BlockSpec((tile, f), lambda t: (t, 0)),
            pl.BlockSpec((tile, d), lambda t: (t, 0)),
            pl.BlockSpec((f, d), lambda t: (0, 0), pipeline_mode=pl.Buffered(1)),
            any_,
        ],
        out_specs=[pl.BlockSpec((tile, d), lambda t: (t, 0)), any_],
        scratch_shapes=gather_sems(2),
        compiler_params=pltpu.CompilerParams(collective_id=1, has_side_effects=True, vmem_limit_bytes=LIMIT, dimension_semantics=("arbitrary",)),
        cost_estimate=pl.CostEstimate(flops=2 * tokens * d * f, bytes_accessed=37_000_000, transcendentals=0),
        name="down",
    )(hid, h, w, wd)


def last_kernel(h_ref, dy_ref, wg_ref, wu_ref, wd_ref, hid_ref, dg_ref, du_ref, at_ref, dyt_ref, dh_ref, dht_ref, gt, ut, dt):
    h = wide(h_ref[...])
    scale = scale_of(h)
    a = (h * scale).astype(BF)
    dy = dy_ref[...]
    f = wg_ref.shape[1]

    @pl.when(pl.program_id(0) == 0)
    def _():
        for n in range(0, f, 256):
            where = slice(n, n + 256)
            gt[where, :] = wg_ref[:, where].T
            ut[where, :] = wu_ref[:, where].T
            dt[:, where] = wd_ref[where, :].T

    at_ref[...] = a.T
    dyt_ref[...] = dy.T
    by_a = jnp.zeros(h.shape, F32)
    for n in range(0, f, 768):
        for k in range(n, n + 768, 256):
            where = slice(k, k + 256)
            g = dot(a, wg_ref[:, where])
            u = dot(a, wu_ref[:, where])
            back = wide(dot(dy, dt[:, where]).astype(BF))
            s = sigmoid(g)
            silu = g * s
            hid_ref[:, where] = (silu * u).astype(BF)
            du_ref[:, where] = (back * silu).astype(BF)
            dg_ref[:, where] = (back * u * (s * (1.0 + g * (1.0 - s)))).astype(BF)
        where = slice(n, n + 768)
        by_a += dot(dg_ref[:, where], gt[where, :]) + dot(du_ref[:, where], ut[where, :])
    by_a = wide(by_a.astype(BF))
    mean = jnp.mean(by_a * h, -1, keepdims=True)
    by_h = (by_a * scale - h * (scale * scale * scale * mean)).astype(BF)
    by_h = dy + by_h
    dh_ref[...] = by_h
    dht_ref[...] = by_h.T


def last_layer(h, dy, wg, wu, wd):
    tokens, d = h.shape
    f = wg.shape[1]
    tile = 512
    rows = lambda n: pl.BlockSpec((tile, n), lambda t: (t, 0))
    columns = pl.BlockSpec((d, tile), lambda t: (0, t))
    fixed = lambda m, n: pl.BlockSpec((m, n), lambda t: (0, 0), pipeline_mode=pl.Buffered(1))
    shape = lambda *s: jax.ShapeDtypeStruct(s, BF)
    return pl.pallas_call(
        last_kernel,
        grid=(tokens // tile,),
        out_shape=[shape(tokens, f)] * 3 + [shape(d, tokens)] * 2 + [shape(tokens, d), shape(d, tokens)],
        in_specs=[rows(d), rows(d), fixed(d, f), fixed(d, f), fixed(f, d)],
        out_specs=[rows(f)] * 3 + [columns] * 2 + [rows(d), columns],
        scratch_shapes=[pltpu.VMEM((f, d), BF)] * 2 + [pltpu.VMEM((d, f), BF)],
        compiler_params=pltpu.CompilerParams(vmem_limit_bytes=LIMIT, dimension_semantics=("arbitrary",)),
        cost_estimate=pl.CostEstimate(flops=10 * tokens * d * f, bytes_accessed=110_000_000, transcendentals=tokens * f),
        name="last_layer",
    )(h, dy, wg, wu, wd)


class Sum:
    COPIES = 7

    def __init__(self, place, store, out, squares, columns, x_first, send, recv):
        self.p, self.out, self.squares, self.x_first = place, out, squares, x_first
        self.term, self.rc, self.sx, self.rx, self.sy, self.ry, self.sz, self.rz = store
        self.rows = self.term.shape[0] // 8
        self.c0, self.width = columns
        self.cols = pl.ds(self.c0, self.width)
        self.send, self.recv = send, recv
        s = place.s
        self.x, self.y, self.core = s // 4, (s // 2) % 2, s % 2

    def chip(self, near, far):
        return near * 2 + far if self.x_first else far * 2 + near

    def block(self, chip, core):
        return pl.ds(pl.multiple_of((chip * 2 + core) * self.rows, 16), self.rows)

    def copy(self, k):
        core, xn, yn, zn, _ = self.p.neighbours()
        first, second = (xn, yn) if self.x_first else (yn, xn)
        if k < 4:
            source, target, device = self.term.at[self.block(k, 1 - self.core), self.cols], self.rc.at[k, :, self.cols], core
        elif k == 4:
            source, target, device = self.sx.at[:, :, self.cols], self.rx.at[:, :, self.cols], first
        elif k == 5:
            source, target, device = self.sy.at[:, self.cols], self.ry.at[:, self.cols], second
        else:
            source, target, device = self.sz.at[:, self.cols], self.rz.at[:, self.cols], zn
        return pltpu.make_async_remote_copy(
            src_ref=source, dst_ref=target, send_sem=self.send.at[k], recv_sem=self.recv.at[k], device_id=device, device_id_type=MESH
        )

    def mine(self, chip, r):
        start = pl.multiple_of((chip * 2 + self.core) * self.rows + r * 16, 16)
        return wide(self.term[pl.ds(start, 16), self.cols]) + wide(self.rc[chip, pl.ds(pl.multiple_of(r * 16, 16), 16), self.cols])

    def each(self, body):
        def go(r, carry):
            body(r, pl.ds(pl.multiple_of(r * 16, 16), 16))
            return carry

        lax.fori_loop(0, self.rows // 16, go, 0)

    def stage0(self):
        for k in range(4):
            self.copy(k).start()

    def stage1(self):
        for k in range(4):
            self.copy(k).wait_recv()
        near = (1 - self.x) if self.x_first else (1 - self.y)

        def body(r, rows):
            for far in range(2):
                self.sx[far, rows, self.cols] = self.mine(self.chip(near, far), r).astype(BF)

        self.each(body)
        self.copy(4).start()

    def stage2(self):
        self.copy(4).wait_recv()
        near, far = (self.x, 1 - self.y) if self.x_first else (self.y, 1 - self.x)

        def body(r, rows):
            self.sy[rows, self.cols] = (self.mine(self.chip(near, far), r) + wide(self.rx[far, rows, self.cols])).astype(BF)

        self.each(body)
        self.copy(5).start()

    def stage3(self):
        self.copy(5).wait_recv()
        for k in range(4):
            self.copy(k).wait_send()
        near, far = (self.x, self.y) if self.x_first else (self.y, self.x)

        def body(r, rows):
            total = self.mine(self.chip(near, far), r) + wide(self.rx[far, rows, self.cols]) + wide(self.ry[rows, self.cols])
            self.sz[rows, self.cols] = total.astype(BF)

        self.each(body)
        self.copy(6).start()

    def stage4(self):
        self.copy(6).wait_recv()

        def body(r, rows):
            total = (wide(self.sz[rows, self.cols]) + wide(self.rz[rows, self.cols])).astype(BF)
            self.out[rows, self.cols] = total
            square = wide(total) * wide(total)
            square = square[:8] + square[8:]
            part = square[:, :LANES]
            for k in range(LANES, self.width, LANES):
                part = part + square[:, k : k + LANES]
            self.squares[...] += part

        self.each(body)
        for k in range(4, self.COPIES):
            self.copy(k).wait_send()


TILE = 256
CHUNK = 1024


def split(items, *sizes):
    parts = []
    for size in sizes:
        parts.append(items[:size])
        items = items[size:]
    return parts, items


def gradients_kernel(phases, pieces, tiles, *refs):
    (lefts, rights, (dh, gate, up, down), outs, (total_ref, dg, du)), rest = split(refs, 4, 4, 4, len(phases), 3)
    rights = (*rights, dg, du)
    left, right, l_sem, r_sem, dh_vmem, w_vmem, in_vmem, out_vmem, dh_sem, w_sem, in_sem, out_sem, *rest = rest
    stores = [rest[8 * i : 8 * i + 8] for i in range(3)]
    squares, parts, send, recv, psend, precv, free = rest[24:]
    place = Place()
    s, z = place.s, place.z
    barrier = pltpu.get_barrier_semaphore()
    peers = [(s + k) % 8 for k in range(1, 8)]
    for peer in peers:
        pl.semaphore_signal(barrier, inc=1, device_id={"s": peer}, device_id_type=MESH)
    pl.semaphore_signal(barrier, inc=1, device_id={"r": 1 - z}, device_id_type=MESH)
    pl.semaphore_wait(barrier, 8)

    sums = [Sum(place, stores[p["store"]], outs[p["phase"]], squares, p["columns"], p["x_first"], send.at[q], recv.at[q]) for q, p in enumerate(pieces)]
    neighbours = place.neighbours()[:4]

    def give(pair):
        for d, device in enumerate(neighbours):
            pl.semaphore_signal(free.at[pair, d], inc=1, device_id=device, device_id_type=MESH)

    def take(pair):
        for d in range(4):
            pl.semaphore_wait(free.at[pair, d], 1)

    def load_left(k):
        return pltpu.make_async_copy(lefts[k], left.at[k % 2], l_sem.at[k % 2])

    def load_right(phase, i, slot):
        cols = pl.ds(pl.multiple_of(i * TILE, TILE), TILE)
        return pltpu.make_async_copy(rights[phase].at[:, cols], right.at[slot], r_sem.at[slot])

    chunks = dh.shape[0] // CHUNK

    def load_dh(n):
        return pltpu.make_async_copy(dh.at[pl.ds(n * CHUNK, CHUNK)], dh_vmem, dh_sem)

    def chunk_at(n, i):
        return pl.ds(n * CHUNK, CHUNK), pl.ds(pl.multiple_of(i * TILE, TILE), TILE)

    def load_chunk(n, i, slot):
        rows, cols = chunk_at(n, i)
        pairs = [(gate.at[rows, cols], in_vmem.at[slot, 0]), (up.at[rows, cols], in_vmem.at[slot, 1])]
        copies = [pltpu.make_async_copy(a, b, in_sem.at[slot, k]) for k, (a, b) in enumerate(pairs)]
        return [*copies, pltpu.make_async_copy(down.at[cols], w_vmem.at[slot], w_sem.at[slot])]

    def store_chunk(n, i, slot):
        rows, cols = chunk_at(n, i)
        return [pltpu.make_async_copy(out_vmem.at[slot, k], ref.at[rows, cols], out_sem.at[slot, k]) for k, ref in enumerate((dg, du))]

    def do(copies, what):
        for copy in copies:
            getattr(copy, what)()

    squares[...] = jnp.zeros_like(squares)
    load_dh(0).start()
    load_left(0).start()
    do(load_chunk(0, 0, 0), "start")
    do(load_chunk(0, 1, 1), "start")
    load_right(0, 0, 0).start()
    load_left(1).start()
    load_right(0, 1, 1).start()
    at = {}
    for q, p in enumerate(pieces):
        for stage, step in enumerate(p["steps"]):
            at.setdefault(step, []).append((q, stage))

    def run(q, stage):
        p = pieces[q]
        if stage == 0 and p["take"] is not None:
            take(p["take"])
        getattr(sums[q], f"stage{stage}")()
        if stage == 4 and p["give"] is not None:
            give(p["give"])

    slots = 2
    for n, (which, turned, store, loads) in enumerate(phases):
        if n == 0 or phases[n - 1][0] != which:
            load_left(which).wait()
        if loads is not None:
            load_left(loads).start()
        term = stores[store][0]
        if n < chunks:
            load_dh(n).wait()

        def tile(i, carry, n=n, which=which, turned=turned, term=term):
            for k in range(tiles):
                if n * tiles + k in at:
                    on(i == k, *[functools.partial(run, q, stage) for q, stage in at[n * tiles + k]])
            slot = (n * tiles + i) % slots
            load_right(n, i, slot).wait()
            if n < chunks:
                do(load_chunk(n, i, slot), "wait")
                on(n * tiles + i >= slots, lambda: do(store_chunk(n, i, slot), "wait"))
                back = wide(dot(dh_vmem[...], w_vmem[slot], ((1,), (1,))).astype(BF))
                g, u = in_vmem[slot, 0], in_vmem[slot, 1]
                sg = sigmoid(g)
                out_vmem[slot, 0] = (back * u * (sg * (1.0 + g * (1.0 - sg)))).astype(BF)
                out_vmem[slot, 1] = (back * (g * sg)).astype(BF)
            total = dot(left[which % 2], right[slot])
            where = pl.ds(pl.multiple_of(i * TILE, TILE), TILE)
            if turned:
                term[where, :] = total.T.astype(BF)
            else:
                term[:, where] = total.astype(BF)

            if n < chunks:
                do(store_chunk(n, i, slot), "start")

            @pl.when(i + slots < tiles)
            def _():
                load_right(n, i + slots, slot).start()
                if n < chunks:
                    do(load_chunk(n, i + slots, slot), "start")

            if n + 1 < len(phases):

                @pl.when(i + slots >= tiles)
                def _():
                    load_right(n + 1, i + slots - tiles, slot).start()
                    if n + 1 < chunks:
                        do(load_chunk(n + 1, i + slots - tiles, slot), "start")

            return carry

        lax.fori_loop(0, tiles, tile, 0)
        if n + 1 < chunks:
            load_dh(n + 1).start()
        if n + 1 == chunks:
            for i in range(tiles - slots, tiles):
                do(store_chunk(n, i, (n * tiles + i) % slots), "wait")

    for step in sorted(at):
        if step >= len(phases) * tiles:
            for q, stage in at[step]:
                run(q, stage)

    def share(k):
        return pltpu.make_async_remote_copy(
            src_ref=squares,
            dst_ref=parts.at[s],
            send_sem=psend.at[k - 1],
            recv_sem=precv.at[k - 1],
            device_id={"s": peers[k - 1]},
            device_id_type=MESH,
        )

    for k in range(1, 8):
        share(k).start()
    parts[s] = squares[...]
    for k in range(1, 8):
        share(k).wait()
    total = parts[0]
    for k in range(1, 8):
        total = total + parts[k]
    total_ref[...] = total


def gradients(lefts, rights, dh, gate, up, down):
    d, tokens = lefts[0].shape
    f = rights[0].shape[1]
    tiles = f // TILE
    phases = [(0, True, 2, None), (1, False, 0, 2), (1, False, 1, None), (2, True, 2, 3), (3, False, 0, None), (3, False, 1, None)]
    gives, takes = {0: 2, 1: 0, 2: 1}, {3: 2, 4: 0, 5: 1}
    pieces = []
    for phase, (_, turned, store_of, _) in enumerate(phases):
        final = phase == len(phases) - 1
        columns = d if turned else f
        cuts = [0, 3 * TILE, 6 * TILE, columns - TILE, columns] if final else [0, -(-columns // 2 // LANES) * LANES, columns]
        gaps = (0, 3, 10, 16, 21) if final else (0, 3, 9, 15, 20)
        for n, (a, b) in enumerate(zip(cuts, cuts[1:])):
            ready = phase * tiles + (tiles if turned else -(-b // TILE))
            pieces.append(
                dict(
                    phase=phase,
                    store=store_of,
                    columns=(a, b - a),
                    x_first=n % 2 == 0,
                    steps=[ready + gap for gap in gaps],
                    take=takes.get(phase) if a == 0 else None,
                    give=gives.get(phase) if b == columns else None,
                )
            )
    shape = lambda *s: pltpu.VMEM(s, BF)

    def store(rows, columns):
        return [
            shape(8 * rows, columns),
            shape(4, rows, columns),
            shape(2, rows, columns),
            shape(2, rows, columns),
            *[shape(rows, columns)] * 4,
        ]

    any_ = pl.BlockSpec(memory_space=pl.ANY)
    vmem = pl.BlockSpec(memory_space=pltpu.VMEM)
    blocks = [jax.ShapeDtypeStruct((f // 8, d) if turned else (d // 8, f), BF) for _, turned, _, _ in phases]
    return pl.pallas_call(
        functools.partial(gradients_kernel, phases, pieces, tiles),
        out_shape=blocks + [jax.ShapeDtypeStruct((8, LANES), F32)] + [jax.ShapeDtypeStruct((tokens, f), BF)] * 2,
        in_specs=[any_] * 12,
        out_specs=[vmem] * 7 + [any_] * 2,
        scratch_shapes=[
            pltpu.VMEM((2, d, tokens), BF),
            pltpu.VMEM((2, tokens, TILE), BF),
            pltpu.SemaphoreType.DMA((2,)),
            pltpu.SemaphoreType.DMA((2,)),
            pltpu.VMEM((CHUNK, d), BF),
            pltpu.VMEM((2, TILE, d), BF),
            pltpu.VMEM((2, 2, CHUNK, TILE), F32),
            pltpu.VMEM((2, 2, CHUNK, TILE), BF),
            pltpu.SemaphoreType.DMA,
            pltpu.SemaphoreType.DMA((2,)),
            pltpu.SemaphoreType.DMA((2, 2)),
            pltpu.SemaphoreType.DMA((2, 2)),
            *store(d // 8, f),
            *store(d // 8, f),
            *store(f // 8, d),
            pltpu.VMEM((8, LANES), F32),
            pltpu.VMEM((8, 8, LANES), F32),
            pltpu.SemaphoreType.DMA((len(pieces), Sum.COPIES)),
            pltpu.SemaphoreType.DMA((len(pieces), Sum.COPIES)),
            pltpu.SemaphoreType.DMA((7,)),
            pltpu.SemaphoreType.DMA((7,)),
            pltpu.SemaphoreType.REGULAR((3, 4)),
        ],
        compiler_params=pltpu.CompilerParams(collective_id=2, has_side_effects=True, vmem_limit_bytes=67_043_328),
        cost_estimate=pl.CostEstimate(flops=14 * tokens * d * f, bytes_accessed=270_000_000, transcendentals=tokens * f),
        name="gradients",
    )(*lefts, *rights, dh, gate, up, down)


def adamw(w, m, v, g):
    m = 0.9 * m + 0.1 * g
    v = 0.95 * v + 0.05 * g * g
    step = m * lax.rsqrt(v + 1e-8) + 0.1 * w
    return (w - 0.02 * step).astype(jnp.bfloat16), m, v


def solution(mesh):
    def step(x, dy, *arrays):
        weights, m, v = (arrays[i : i + 3] for i in (0, 3, 6))
        wg, wu, wd = weights
        x, dy = x[0], dy[0]
        g, u, hid0, at0, wd0, wg1, wu1 = gate_up(x, wg, wu, wd)
        h, wd1 = down(hid0, x, wd0, wd)
        hid1, dg1, du1, at1, dyt, dh, dht = last_layer(h, dy, wg1, wu1, wd1)
        d1, g1, u1, d0, g0, u0, squares, *_ = gradients((dyt, at1, dht, at0), (hid1, dg1, du1, hid0), dh, g, u, wd0)
        own = [jnp.stack(pair).astype(F32) for pair in ((g0, g1), (u0, u1), (d0, d1))]
        count = lax.psum(1, "s") * sum(g.size for g in own)
        factor = jnp.minimum(1.0, 0.5 * lax.rsqrt(jnp.sum(squares) / count + 1e-30))
        new = [adamw(w.astype(F32), m, v, g * factor) for w, m, v, g in zip(weights, m, v, own, strict=True)]
        return tuple(one[which] for which in range(3) for one in new)

    states, cut = P(("rep", "r", "s"), None, None), P(None, "s", None)
    return jax.shard_map(
        step,
        mesh=mesh,
        in_specs=(states, states) + (cut,) * 9,
        out_specs=(P("rep", "s", None),) * 9,
        check_vma=False,
    )
```

```python
import functools

import jax
import jax.numpy as jnp
from jax import lax
from jax.experimental import pallas as pl
from jax.experimental.pallas import tpu as pltpu
from jax.sharding import PartitionSpec as P

NAMES = ("w_gate", "w_up", "w_down")
MESH = pl.DeviceIdType.MESH
BF, F32 = jnp.bfloat16, jnp.float32
LIMIT = 60 * 1024 * 1024
LANES = 128


def wide(a):
    return a.astype(F32)


def dot(a, b, contract=((1,), (0,))):
    return lax.dot_general(a, b, (contract, ((), ())), preferred_element_type=F32)


def scale_of(h):
    return lax.rsqrt(jnp.mean(h * h, -1, keepdims=True) + 1e-6)


class Place:
    def __init__(self):
        s = lax.axis_index("s")
        x, y, core = s // 4, (s // 2) % 2, s % 2
        at = lambda x, y, core: x * 4 + y * 2 + core
        self.s, self.z = s, lax.axis_index("r")
        self.other, self.xn, self.yn, self.diagonal = at(x, y, 1 - core), at(1 - x, y, core), at(x, 1 - y, core), at(1 - x, 1 - y, core)

    def neighbours(self):
        return ({"s": self.other}, {"s": self.xn}, {"s": self.yn}, {"r": 1 - self.z}, {"s": self.diagonal})

    def barrier(self):
        barrier = pltpu.get_barrier_semaphore()
        for device in self.neighbours():
            pl.semaphore_signal(barrier, inc=1, device_id=device, device_id_type=MESH)
        pl.semaphore_wait(barrier, len(self.neighbours()))


TRANSFERS = 13


class Gather:
    def __init__(self, place, block, whole, axis, sems):
        self.p, self.block, self.whole, self.axis = place, block, whole, axis
        self.rows = block.shape[0]
        size = block.shape[axis]
        grain = LANES if axis else 16
        self.half = size // 2
        self.first = (self.half // grain + 1) // 2 * grain
        self.send, self.recv, self.local = sems
        core, xn, yn, zn, diagonal = place.neighbours()
        z, inner = place.z, size - self.first
        most, half = (z * self.first, inner), (z * self.half, self.half)
        edge, edge2 = (z * inner, self.first), ((1 - z) * inner, self.first)
        own, x, y, d = place.s, place.xn, place.yn, place.diagonal
        half2 = ((1 - z) * self.half, self.half)
        every = [(own, (0, size), core), (own, most, xn), (own, most, yn), (own, half, diagonal)]
        every += [(x, most, core), (y, most, core), (d, half, core), (x, edge, zn), (y, edge, zn), (d, half, zn)]
        every += [(x, edge2, core), (y, edge2, core), (d, half2, core)]
        self.every = every

    def part(self, ref, s, offset, size):
        start = 0 if s is None else pl.multiple_of(s * self.rows, 16)
        if self.axis:
            return ref.at[pl.ds(start, self.rows), pl.ds(pl.multiple_of(offset, LANES), size)]
        return ref.at[pl.ds(start + pl.multiple_of(offset, 16), size)]

    def copy(self, k):
        s, (offset, size), device = self.every[k]
        target = self.part(self.whole, s, offset, size)
        source = self.part(self.block, None, offset, size) if s is self.p.s else target
        return pltpu.make_async_remote_copy(
            src_ref=source, dst_ref=target, send_sem=self.send.at[k], recv_sem=self.recv.at[k], device_id=device, device_id_type=MESH
        )

    def keep(self):
        return pltpu.make_async_copy(self.block, self.whole.at[pl.ds(pl.multiple_of(self.p.s * self.rows, 16), self.rows)], self.local)

    def start(self):
        for k in (1, 2, 3, 0):
            self.copy(k).start()
        self.keep().start()

    def second(self):
        for k in (1, 2, 3):
            self.copy(k).wait_recv()
        for k in (7, 8, 9, 4, 5, 6):
            self.copy(k).start()

    def third(self):
        for k in (7, 8, 9):
            self.copy(k).wait_recv()
            self.copy(k + 3).start()

    def finish(self):
        for k in (0, 4, 5, 6, 10, 11, 12):
            self.copy(k).wait_recv()
        for k in range(TRANSFERS):
            self.copy(k).wait_send()
        self.keep().wait()


def gather_sems(jobs):
    return [pltpu.SemaphoreType.DMA((jobs, TRANSFERS)), pltpu.SemaphoreType.DMA((jobs, TRANSFERS)), pltpu.SemaphoreType.DMA((jobs,))]


def on(step, *actions):
    @pl.when(step)
    def _():
        for action in actions:
            action()


def sigmoid(x):
    return 0.5 * jnp.tanh(0.5 * x) + 0.5


def gate_up_kernel(parts, tiles, h_ref, wg_ref, wu_ref, wd_ref, g_ref, u_ref, hid_ref, at_ref, wd0_ref, wg1_ref, wu1_ref, wg, wu, send, recv, local):
    part, tile = pl.program_id(0), pl.program_id(1)
    step = part * tiles + tile
    place = Place()
    width = g_ref.shape[1]
    f = wg_ref.shape[2]
    middle = (f // LANES + 2) // 4 * 2 * LANES
    ranges = [(own.at[0], whole, pl.ds(n * width, width), 1) for n in range(parts) for own, whole in ((wg_ref, wg), (wu_ref, wu))]
    ranges += [(wd_ref.at[0], wd0_ref, pl.ds(0, wd_ref.shape[2]), 0), (wg_ref.at[1], wg1_ref, pl.ds(0, f), 1)]
    ranges += [(wu_ref.at[1], wu1_ref, cols, 1) for cols in (pl.ds(0, middle), pl.ds(middle, f - middle))]
    jobs = [
        Gather(place, own.at[:, cols], whole.at[:, cols], axis, (send.at[k], recv.at[k], local.at[k])) for k, (own, whole, cols, axis) in enumerate(ranges)
    ]
    b0, b1, b2, (down, gate1), up1 = [jobs[k : k + 2] for k in range(0, len(jobs), 2)]
    both = lambda pair, *stages: [getattr(job, stage) for stage in stages for job in pair]
    last = parts * tiles - 1

    on(step == 0, place.barrier, *both(b0, "start"), *both(b1, "start"), *both(b0, "second", "third", "finish"), *both(b2, "start"))
    on(step == 1, *both(b1, "second"), down.start)
    on(step == 5, *both(b2, "second"), gate1.start)
    on(step == 6, *both(b1, "third"))
    on(step == tiles, *both(b1, "finish"))
    on(step == 10, *both(b2, "third"), down.second)
    on(step == 11, *both(up1, "start"))
    on(step == 2 * tiles, *both(b2, "finish"), down.third, gate1.second)
    on(step == 18, down.finish)
    on(step == 20, up1[0].second)
    on(step == 22, gate1.third)
    on(step == last, gate1.finish, up1[1].second)

    h = wide(h_ref[...])
    a = (h * scale_of(h)).astype(BF)

    @pl.when(part == 0)
    def _():
        at_ref[...] = a.T

    for n in range(0, width, 256):
        where = pl.ds(pl.multiple_of(part * width + n, LANES), 256)
        g = dot(a, wg[:, where])
        u = dot(a, wu[:, where])
        g_ref[:, n : n + 256] = g
        u_ref[:, n : n + 256] = u
        hid_ref[:, n : n + 256] = (g * sigmoid(g) * u).astype(BF)

    on(step == last, *both(up1, "third", "finish"))


def gate_up(h, wg, wu, wd):
    tokens, d = h.shape
    _, rows, f = wg.shape
    parts, tile = 3, 512
    width, tiles = f // parts, tokens // tile
    group = d // rows
    any_ = pl.BlockSpec(memory_space=pl.ANY)
    return pl.pallas_call(
        functools.partial(gate_up_kernel, parts, tiles),
        grid=(parts, tiles),
        out_shape=[
            jax.ShapeDtypeStruct((tokens, f), F32),
            jax.ShapeDtypeStruct((tokens, f), F32),
            jax.ShapeDtypeStruct((tokens, f), BF),
            jax.ShapeDtypeStruct((d, tokens), BF),
            jax.ShapeDtypeStruct((wd.shape[1] * group, d), BF),
            jax.ShapeDtypeStruct((d, f), BF),
            jax.ShapeDtypeStruct((d, f), BF),
        ],
        in_specs=[pl.BlockSpec((tile, d), lambda p, t: (t, 0)), any_, any_, any_],
        out_specs=[pl.BlockSpec((tile, width), lambda p, t: (t, p))] * 3
        + [pl.BlockSpec((d, tile), lambda p, t: (0, jnp.where(p == 0, t, tiles - 1))), any_, any_, any_],
        scratch_shapes=[pltpu.VMEM((d, f), BF)] * 2 + gather_sems(2 * parts + 4),
        compiler_params=pltpu.CompilerParams(
            collective_id=0, has_side_effects=True, vmem_limit_bytes=LIMIT, dimension_semantics=("arbitrary", "arbitrary")
        ),
        cost_estimate=pl.CostEstimate(flops=4 * tokens * d * f, bytes_accessed=110_000_000, transcendentals=tokens * f),
        name="gate_up",
    )(h, wg, wu, wd)


def down_kernel(tiles, hid_ref, h_ref, w_ref, wd_ref, h1_ref, wd1_ref, send, recv, local):
    step = pl.program_id(0)
    place = Place()
    d = wd_ref.shape[2]
    middle = (d // LANES + 1) // 2 * LANES
    jobs = [
        Gather(place, wd_ref.at[1, :, cols], wd1_ref.at[:, cols], 0, (send.at[k], recv.at[k], local.at[k]))
        for k, cols in enumerate((pl.ds(0, middle), pl.ds(middle, d - middle)))
    ]
    on(step == 0, place.barrier, *[job.start for job in jobs])
    on(step == tiles - 3, jobs[0].second)
    on(step == tiles - 1, jobs[1].second)
    h1_ref[...] = h_ref[...] + dot(hid_ref[...], w_ref[...]).astype(BF)
    on(step == tiles - 1, *[job.third for job in jobs], *[job.finish for job in jobs])


def down(hid, h, w, wd):
    tokens, d = h.shape
    f = hid.shape[1]
    tile = 512
    any_ = pl.BlockSpec(memory_space=pl.ANY)
    return pl.pallas_call(
        functools.partial(down_kernel, tokens // tile),
        grid=(tokens // tile,),
        out_shape=[jax.ShapeDtypeStruct((tokens, d), BF), jax.ShapeDtypeStruct((f, d), BF)],
        in_specs=[
            pl.BlockSpec((tile, f), lambda t: (t, 0)),
            pl.BlockSpec((tile, d), lambda t: (t, 0)),
            pl.BlockSpec((f, d), lambda t: (0, 0), pipeline_mode=pl.Buffered(1)),
            any_,
        ],
        out_specs=[pl.BlockSpec((tile, d), lambda t: (t, 0)), any_],
        scratch_shapes=gather_sems(2),
        compiler_params=pltpu.CompilerParams(collective_id=1, has_side_effects=True, vmem_limit_bytes=LIMIT, dimension_semantics=("arbitrary",)),
        cost_estimate=pl.CostEstimate(flops=2 * tokens * d * f, bytes_accessed=37_000_000, transcendentals=0),
        name="down",
    )(hid, h, w, wd)


def last_kernel(h_ref, dy_ref, wg_ref, wu_ref, wd_ref, hid_ref, dg_ref, du_ref, at_ref, dyt_ref, dh_ref, dht_ref):
    h = wide(h_ref[...])
    scale = scale_of(h)
    a = (h * scale).astype(BF)
    dy = dy_ref[...]
    f = wg_ref.shape[1]
    at_ref[...] = a.T
    dyt_ref[...] = dy.T
    for k in range(0, f, 256):
        where = slice(k, k + 256)
        g = dot(a, wg_ref[:, where])
        u = dot(a, wu_ref[:, where])
        back = wide(dot(dy, wd_ref[where, :], ((1,), (1,))).astype(BF))
        s = sigmoid(g)
        silu = g * s
        hid_ref[:, where] = (silu * u).astype(BF)
        du_ref[:, where] = (back * silu).astype(BF)
        dg_ref[:, where] = (back * u * (s * (1.0 + g * (1.0 - s)))).astype(BF)
    d = h.shape[1]
    parts = []
    for k in range(0, d, 256):
        rows = slice(k, min(k + 256, d))
        parts.append(dot(dg_ref[...], wg_ref[rows, :], ((1,), (1,))) + dot(du_ref[...], wu_ref[rows, :], ((1,), (1,))))
    by_a = jnp.concatenate(parts, 1)
    by_a = wide(by_a.astype(BF))
    mean = jnp.mean(by_a * h, -1, keepdims=True)
    by_h = (by_a * scale - h * (scale * scale * scale * mean)).astype(BF)
    by_h = dy + by_h
    dh_ref[...] = by_h
    dht_ref[...] = by_h.T


def last_layer(h, dy, wg, wu, wd):
    tokens, d = h.shape
    f = wg.shape[1]
    tile = 512
    rows = lambda n: pl.BlockSpec((tile, n), lambda t: (t, 0))
    columns = pl.BlockSpec((d, tile), lambda t: (0, t))
    fixed = lambda m, n: pl.BlockSpec((m, n), lambda t: (0, 0), pipeline_mode=pl.Buffered(1))
    shape = lambda *s: jax.ShapeDtypeStruct(s, BF)
    return pl.pallas_call(
        last_kernel,
        grid=(tokens // tile,),
        out_shape=[shape(tokens, f)] * 3 + [shape(d, tokens)] * 2 + [shape(tokens, d), shape(d, tokens)],
        in_specs=[rows(d), rows(d), fixed(d, f), fixed(d, f), fixed(f, d)],
        out_specs=[rows(f)] * 3 + [columns] * 2 + [rows(d), columns],
        compiler_params=pltpu.CompilerParams(vmem_limit_bytes=LIMIT, dimension_semantics=("arbitrary",)),
        cost_estimate=pl.CostEstimate(flops=10 * tokens * d * f, bytes_accessed=110_000_000, transcendentals=tokens * f),
        name="last_layer",
    )(h, dy, wg, wu, wd)


class Sum:
    COPIES = 7

    def __init__(self, place, store, out, squares, columns, x_first, send, recv):
        self.p, self.out, self.squares, self.x_first = place, out, squares, x_first
        self.term, self.rc, self.sx, self.rx, self.sy, self.ry, self.sz, self.rz = store
        self.rows = self.term.shape[0] // 8
        self.c0, self.width = columns
        self.cols = pl.ds(self.c0, self.width)
        self.send, self.recv = send, recv
        s = place.s
        self.x, self.y, self.core = s // 4, (s // 2) % 2, s % 2

    def chip(self, near, far):
        return near * 2 + far if self.x_first else far * 2 + near

    def block(self, chip, core):
        return pl.ds(pl.multiple_of((chip * 2 + core) * self.rows, 16), self.rows)

    def copy(self, k):
        core, xn, yn, zn, _ = self.p.neighbours()
        first, second = (xn, yn) if self.x_first else (yn, xn)
        if k < 4:
            source, target, device = self.term.at[self.block(k, 1 - self.core), self.cols], self.rc.at[k, :, self.cols], core
        elif k == 4:
            source, target, device = self.sx.at[:, :, self.cols], self.rx.at[:, :, self.cols], first
        elif k == 5:
            source, target, device = self.sy.at[:, self.cols], self.ry.at[:, self.cols], second
        else:
            source, target, device = self.sz.at[:, self.cols], self.rz.at[:, self.cols], zn
        return pltpu.make_async_remote_copy(
            src_ref=source, dst_ref=target, send_sem=self.send.at[k], recv_sem=self.recv.at[k], device_id=device, device_id_type=MESH
        )

    def mine(self, chip, r):
        start = pl.multiple_of((chip * 2 + self.core) * self.rows + r * 16, 16)
        return wide(self.term[pl.ds(start, 16), self.cols]) + wide(self.rc[chip, pl.ds(pl.multiple_of(r * 16, 16), 16), self.cols])

    def each(self, body):
        def go(r, carry):
            body(r, pl.ds(pl.multiple_of(r * 16, 16), 16))
            return carry

        lax.fori_loop(0, self.rows // 16, go, 0)

    def stage0(self):
        for k in range(4):
            self.copy(k).start()

    def stage1(self):
        for k in range(4):
            self.copy(k).wait_recv()
        near = (1 - self.x) if self.x_first else (1 - self.y)

        def body(r, rows):
            for far in range(2):
                self.sx[far, rows, self.cols] = self.mine(self.chip(near, far), r).astype(BF)

        self.each(body)
        self.copy(4).start()

    def stage2(self):
        self.copy(4).wait_recv()
        near, far = (self.x, 1 - self.y) if self.x_first else (self.y, 1 - self.x)

        def body(r, rows):
            self.sy[rows, self.cols] = (self.mine(self.chip(near, far), r) + wide(self.rx[far, rows, self.cols])).astype(BF)

        self.each(body)
        self.copy(5).start()

    def stage3(self):
        self.copy(5).wait_recv()
        for k in range(4):
            self.copy(k).wait_send()
        near, far = (self.x, self.y) if self.x_first else (self.y, self.x)

        def body(r, rows):
            total = self.mine(self.chip(near, far), r) + wide(self.rx[far, rows, self.cols]) + wide(self.ry[rows, self.cols])
            self.sz[rows, self.cols] = total.astype(BF)

        self.each(body)
        self.copy(6).start()

    def stage4(self):
        self.copy(6).wait_recv()

        def body(r, rows):
            total = (wide(self.sz[rows, self.cols]) + wide(self.rz[rows, self.cols])).astype(BF)
            self.out[rows, self.cols] = total
            square = wide(total) * wide(total)
            square = square[:8] + square[8:]
            part = square[:, :LANES]
            for k in range(LANES, self.width, LANES):
                part = part + square[:, k : k + LANES]
            self.squares[...] += part

        self.each(body)
        for k in range(4, self.COPIES):
            self.copy(k).wait_send()


TILE = 256
CHUNK = 1024


def split(items, *sizes):
    parts = []
    for size in sizes:
        parts.append(items[:size])
        items = items[size:]
    return parts, items


def gradients_kernel(phases, pieces, tiles, *refs):
    (lefts, rights, (dh, gate, up, down), outs, (total_ref, dg, du)), rest = split(refs, 4, 4, 4, len(phases), 3)
    rights = (*rights, dg, du)
    left, right, l_sem, r_sem, dh_vmem, w_vmem, in_vmem, out_vmem, dh_sem, w_sem, in_sem, out_sem, *rest = rest
    stores = [rest[8 * i : 8 * i + 8] for i in range(3)]
    squares, parts, send, recv, psend, precv, free = rest[24:]
    place = Place()
    s, z = place.s, place.z
    barrier = pltpu.get_barrier_semaphore()
    peers = [(s + k) % 8 for k in range(1, 8)]
    for peer in peers:
        pl.semaphore_signal(barrier, inc=1, device_id={"s": peer}, device_id_type=MESH)
    pl.semaphore_signal(barrier, inc=1, device_id={"r": 1 - z}, device_id_type=MESH)
    pl.semaphore_wait(barrier, 8)

    sums = [Sum(place, stores[p["store"]], outs[p["phase"]], squares, p["columns"], p["x_first"], send.at[q], recv.at[q]) for q, p in enumerate(pieces)]
    neighbours = place.neighbours()[:4]

    def give(pair):
        for d, device in enumerate(neighbours):
            pl.semaphore_signal(free.at[pair, d], inc=1, device_id=device, device_id_type=MESH)

    def take(pair):
        for d in range(4):
            pl.semaphore_wait(free.at[pair, d], 1)

    def load_left(k):
        return pltpu.make_async_copy(lefts[k], left.at[k % 2], l_sem.at[k % 2])

    def load_right(phase, i, slot):
        cols = pl.ds(pl.multiple_of(i * TILE, TILE), TILE)
        return pltpu.make_async_copy(rights[phase].at[:, cols], right.at[slot], r_sem.at[slot])

    chunks = dh.shape[0] // CHUNK

    def load_dh(n):
        return pltpu.make_async_copy(dh.at[pl.ds(n * CHUNK, CHUNK)], dh_vmem, dh_sem)

    def chunk_at(n, i):
        return pl.ds(n * CHUNK, CHUNK), pl.ds(pl.multiple_of(i * TILE, TILE), TILE)

    def load_chunk(n, i, slot):
        rows, cols = pl.ds(pl.multiple_of(n * CHUNK, CHUNK), CHUNK), chunk_at(0, i)[1]
        pairs = [(gate.at[rows, cols], in_vmem.at[slot, 0]), (up.at[rows, cols], in_vmem.at[slot, 1])]
        copies = [pltpu.make_async_copy(a, b, in_sem.at[slot, k]) for k, (a, b) in enumerate(pairs)]
        return [*copies, pltpu.make_async_copy(down.at[cols], w_vmem.at[slot], w_sem.at[slot])]

    def store_chunk(n, i, slot):
        rows, cols = chunk_at(n, i)
        return [pltpu.make_async_copy(out_vmem.at[slot, k], ref.at[rows, cols], out_sem.at[slot, k]) for k, ref in enumerate((dg, du))]

    def do(copies, what):
        for copy in copies:
            getattr(copy, what)()

    squares[...] = jnp.zeros_like(squares)
    load_dh(0).start()
    load_left(0).start()
    do(load_chunk(0, 0, 0), "start")
    do(load_chunk(0, 1, 1), "start")
    load_right(0, 0, 0).start()
    load_left(1).start()
    load_right(0, 1, 1).start()
    at = {}
    for q, p in enumerate(pieces):
        for stage, step in enumerate(p["steps"]):
            at.setdefault(step, []).append((q, stage))

    def run(q, stage):
        p = pieces[q]
        if stage == 0 and p["take"] is not None:
            take(p["take"])
        getattr(sums[q], f"stage{stage}")()
        if stage == 4 and p["give"] is not None:
            give(p["give"])

    slots = 2
    for n, (which, turned, store, loads) in enumerate(phases):
        if n == 0 or phases[n - 1][0] != which:
            load_left(which).wait()
        if loads is not None:
            load_left(loads).start()
        term = stores[store][0]
        if n < chunks:
            load_dh(n).wait()

        def tile(i, carry, n=n, which=which, turned=turned, term=term):
            for k in range(tiles):
                if n * tiles + k in at:
                    on(i == k, *[functools.partial(run, q, stage) for q, stage in at[n * tiles + k]])
            slot = (n * tiles + i) % slots
            load_right(n, i, slot).wait()
            if n < chunks:
                do(load_chunk(n, i, slot), "wait")
                on(n * tiles + i >= slots, lambda: do(store_chunk(n, i, slot), "wait"))
                back = wide(dot(dh_vmem[...], w_vmem[slot], ((1,), (1,))).astype(BF))
                g, u = in_vmem[slot, 0], in_vmem[slot, 1]
                sg = sigmoid(g)
                out_vmem[slot, 0] = (back * u * (sg * (1.0 + g * (1.0 - sg)))).astype(BF)
                out_vmem[slot, 1] = (back * (g * sg)).astype(BF)
                if n + 1 < chunks:
                    after = n * tiles + i + slots
                    do(load_chunk(after // tiles, after % tiles, slot), "start")
            total = dot(left[which % 2], right[slot])
            where = pl.ds(pl.multiple_of(i * TILE, TILE), TILE)
            if turned:
                term[where, :] = total.T.astype(BF)
            else:
                term[:, where] = total.astype(BF)

            if n < chunks:
                do(store_chunk(n, i, slot), "start")

            @pl.when(i + slots < tiles)
            def _():
                load_right(n, i + slots, slot).start()
                if n + 1 == chunks:
                    do(load_chunk(n, i + slots, slot), "start")

            if n + 1 < len(phases):

                @pl.when(i + slots >= tiles)
                def _():
                    load_right(n + 1, i + slots - tiles, slot).start()

            return carry

        lax.fori_loop(0, tiles, tile, 0)
        if n + 1 < chunks:
            load_dh(n + 1).start()
        if n + 1 == chunks:
            for i in range(tiles - slots, tiles):
                do(store_chunk(n, i, (n * tiles + i) % slots), "wait")

    for step in sorted(at):
        if step >= len(phases) * tiles:
            for q, stage in at[step]:
                run(q, stage)

    def share(k):
        return pltpu.make_async_remote_copy(
            src_ref=squares,
            dst_ref=parts.at[s],
            send_sem=psend.at[k - 1],
            recv_sem=precv.at[k - 1],
            device_id={"s": peers[k - 1]},
            device_id_type=MESH,
        )

    for k in range(1, 8):
        share(k).start()
    parts[s] = squares[...]
    for k in range(1, 8):
        share(k).wait()
    total = parts[0]
    for k in range(1, 8):
        total = total + parts[k]
    total_ref[...] = total


def gradients(lefts, rights, dh, gate, up, down):
    d, tokens = lefts[0].shape
    f = rights[0].shape[1]
    tiles = f // TILE
    phases = [(0, True, 2, None), (1, False, 0, 2), (1, False, 1, None), (2, True, 2, 3), (3, False, 0, None), (3, False, 1, None)]
    gives, takes = {0: 2, 1: 0, 2: 1}, {3: 2, 4: 0, 5: 1}
    pieces = []
    for phase, (_, turned, store_of, _) in enumerate(phases):
        final = phase == len(phases) - 1
        columns = d if turned else f
        cuts = [0, 3 * TILE, 6 * TILE, columns - TILE, columns] if final else [0, -(-columns // 2 // LANES) * LANES, columns]
        gaps = (0, 3, 10, 16, 21) if final else (0, 3, 9, 15, 20)
        for n, (a, b) in enumerate(zip(cuts, cuts[1:])):
            ready = phase * tiles + (tiles if turned else -(-b // TILE))
            pieces.append(
                dict(
                    phase=phase,
                    store=store_of,
                    columns=(a, b - a),
                    x_first=n % 2 == 0,
                    steps=[ready + gap for gap in gaps],
                    take=takes.get(phase) if a == 0 else None,
                    give=gives.get(phase) if b == columns else None,
                )
            )
    shape = lambda *s: pltpu.VMEM(s, BF)

    def store(rows, columns):
        return [
            shape(8 * rows, columns),
            shape(4, rows, columns),
            shape(2, rows, columns),
            shape(2, rows, columns),
            *[shape(rows, columns)] * 4,
        ]

    any_ = pl.BlockSpec(memory_space=pl.ANY)
    vmem = pl.BlockSpec(memory_space=pltpu.VMEM)
    blocks = [jax.ShapeDtypeStruct((f // 8, d) if turned else (d // 8, f), BF) for _, turned, _, _ in phases]
    return pl.pallas_call(
        functools.partial(gradients_kernel, phases, pieces, tiles),
        out_shape=blocks + [jax.ShapeDtypeStruct((8, LANES), F32)] + [jax.ShapeDtypeStruct((tokens, f), BF)] * 2,
        in_specs=[any_] * 12,
        out_specs=[vmem] * 7 + [any_] * 2,
        scratch_shapes=[
            pltpu.VMEM((2, d, tokens), BF),
            pltpu.VMEM((2, tokens, TILE), BF),
            pltpu.SemaphoreType.DMA((2,)),
            pltpu.SemaphoreType.DMA((2,)),
            pltpu.VMEM((CHUNK, d), BF),
            pltpu.VMEM((2, TILE, d), BF),
            pltpu.VMEM((2, 2, CHUNK, TILE), F32),
            pltpu.VMEM((2, 2, CHUNK, TILE), BF),
            pltpu.SemaphoreType.DMA,
            pltpu.SemaphoreType.DMA((2,)),
            pltpu.SemaphoreType.DMA((2, 2)),
            pltpu.SemaphoreType.DMA((2, 2)),
            *store(d // 8, f),
            *store(d // 8, f),
            *store(f // 8, d),
            pltpu.VMEM((8, LANES), F32),
            pltpu.VMEM((8, 8, LANES), F32),
            pltpu.SemaphoreType.DMA((len(pieces), Sum.COPIES)),
            pltpu.SemaphoreType.DMA((len(pieces), Sum.COPIES)),
            pltpu.SemaphoreType.DMA((7,)),
            pltpu.SemaphoreType.DMA((7,)),
            pltpu.SemaphoreType.REGULAR((3, 4)),
        ],
        compiler_params=pltpu.CompilerParams(collective_id=2, has_side_effects=True, vmem_limit_bytes=67_043_328),
        cost_estimate=pl.CostEstimate(flops=14 * tokens * d * f, bytes_accessed=270_000_000, transcendentals=tokens * f),
        name="gradients",
    )(*lefts, *rights, dh, gate, up, down)


def adamw(w, m, v, g):
    m = 0.9 * m + 0.1 * g
    v = 0.95 * v + 0.05 * g * g
    step = m * lax.rsqrt(v + 1e-8) + 0.1 * w
    return (w - 0.02 * step).astype(jnp.bfloat16), m, v


def solution(mesh):
    def step(x, dy, *arrays):
        weights, m, v = (arrays[i : i + 3] for i in (0, 3, 6))
        wg, wu, wd = weights
        x, dy = x[0], dy[0]
        g, u, hid0, at0, wd0, wg1, wu1 = gate_up(x, wg, wu, wd)
        h, wd1 = down(hid0, x, wd0, wd)
        hid1, dg1, du1, at1, dyt, dh, dht = last_layer(h, dy, wg1, wu1, wd1)
        d1, g1, u1, d0, g0, u0, squares, *_ = gradients((dyt, at1, dht, at0), (hid1, dg1, du1, hid0), dh, g, u, wd0)
        own = [jnp.stack(pair).astype(F32) for pair in ((g0, g1), (u0, u1), (d0, d1))]
        count = lax.psum(1, "s") * sum(g.size for g in own)
        factor = jnp.minimum(1.0, 0.5 * lax.rsqrt(jnp.sum(squares) / count + 1e-30))
        new = [adamw(w.astype(F32), m, v, g * factor) for w, m, v, g in zip(weights, m, v, own, strict=True)]
        return tuple(one[which] for which in range(3) for one in new)

    states, cut = P(("rep", "r", "s"), None, None), P(None, "s", None)
    return jax.shard_map(
        step,
        mesh=mesh,
        in_specs=(states, states) + (cut,) * 9,
        out_specs=(P("rep", "s", None),) * 9,
        check_vma=False,
    )
```
